256 devices in a mesh: box: 256 (over y, z, x, core).
Axes of the slice: x: 4, y: 4, z: 8, core: 2. Of those that a mesh axis runs over, the one named last changes fastest.
Arguments:
- basis_vector: float32 [16, 1048576], P(None, 'box'), may hold values from -600 to 600
- diagonal: float32 [1048576], P('box'), may hold values from 0.25 to 2
- coords: int32 [2, 1048576], P(None, 'box'), may hold values from 0 to 4095
- phase_scale: int32 [1], replicated, may hold values from 1 to 8190
- sketch_rows: int32 [1048576], P('box'), may hold values from 0 to 2047
- sketch_signs: int32 [1048576], P('box'), may hold values from 0 to 1
Outputs:
- new_basis: float32 [16, 1048576], P(None, 'box')
- sketch: float32 [16, 2048], replicated
- arnoldi: float32 [2, 16], replicated
The draws below stay inside these ranges and needn't reach their ends.
All inputs are finite; a program needn't handle non-finite values.
Results may differ from the reference program's by a relative error of at most 0.00019.
Values sent between devices are 32-bit elements; how exact they have to be, the bound alone decides.
No kernel may reach another device: no remote copies, remote signals or barrier semaphores. Data moves between devices by JAX's collectives and lax.ppermute only.
A program may use at most 64 MiB of HBM per device.

```python
import math
import jax
import jax.numpy as jnp
from jax import lax

RANK = 16
WIDTH = 32
LEAF = 32
GRID = 4096
SKETCH = 2048
NRHS = 16
BOX_DEV = 128
NPTS = 1048576
SECTIONS = 8
N_BOX = 256


def draw_basis_vector(key, part):
    key_scale, key_normal = jax.random.split(key, 2)
    position = jnp.arange(NPTS, dtype=jnp.float32) / NPTS
    row_scale = jnp.exp(jax.random.uniform(key_scale, (NPTS,), jnp.float32, 0.0, math.log(10.0))) * jnp.exp(position * math.log(3.0))
    normal_part = jax.random.normal(key_normal, (NRHS, NPTS), jnp.float32)
    return jnp.clip(normal_part, -4.0, 4.0) * row_scale[None, :]


def with_ends(drawn, own_key, low, largest):
    spot = [jax.random.randint(jax.random.fold_in(own_key, axis), (), 0, length) for axis, length in enumerate(drawn.shape)]
    widest = drawn.shape.index(max(drawn.shape))
    next_to = spot[:widest] + [(spot[widest] + 1) % drawn.shape[widest]] + spot[widest + 1:]
    return drawn.at[tuple(spot)].set(low).at[tuple(next_to)].set(largest)


def levels(own_key, shape, pieces, low, top_value):
    gain, own = 1.0, jax.random.fold_in(own_key, 6)
    for dim, shards_of in pieces:
        steps = jnp.exp(jax.random.uniform(jax.random.fold_in(own, dim), (shards_of,), jnp.float32, low / len(pieces), top_value / len(pieces)))
        gain = gain * jnp.repeat(steps, shape[dim] // shards_of).reshape([-1 if axis == dim else 1 for axis in range(len(shape))])
    return gain


def setup_inputs(seed: int = 0) -> dict:
    keys = jax.random.split(jax.random.key(seed), 7)
    basis_vector = draw_basis_vector(jax.random.fold_in(keys[6], 71), 0)
    diagonal = jnp.clip(jnp.exp(math.log(2.0) - 2.0794415 * jax.random.uniform(keys[1], (NPTS,), jnp.float32) ** levels(keys[1], (NPTS,), ((0, 256),), -0.2, 0.2)), 0.25, 2.0)
    coords = with_ends(jax.random.randint(keys[2], (2, NPTS), 0, GRID), jax.random.fold_in(keys[2], 1), 0, GRID - 1).astype(jnp.int32)
    phase_scale = jax.random.randint(keys[3], (1,), 1, 8191).astype(jnp.int32)
    sketch_rows = with_ends(jax.random.randint(keys[4], (NPTS,), 0, SKETCH), jax.random.fold_in(keys[4], 1), 0, SKETCH - 1).astype(jnp.int32)
    sketch_signs = with_ends(jax.random.randint(keys[5], (NPTS,), 0, 2), jax.random.fold_in(keys[5], 1), 0, 1).astype(jnp.int32)
    return {"basis_vector": basis_vector, "diagonal": diagonal, "coords": coords, "phase_scale": phase_scale, "sketch_rows": sketch_rows, "sketch_signs": sketch_signs}


modulus = 8191
epsilon = 1e-06

def leaf_table(coords, phase_scale):
    scale_mod = phase_scale[0] % modulus
    freq = jnp.arange(RANK, dtype=jnp.int32)
    freq_first = freq % 4 + 1
    freq_second = freq // 4 + 1
    linear = (freq_first[:, None] * coords[0][None, :] + freq_second[:, None] * coords[1][None, :]) % modulus
    phase = scale_mod * linear % modulus
    angle = phase.astype(jnp.float32) * (2.0 * math.pi / modulus)
    return jnp.concatenate([jnp.cos(angle), jnp.sin(angle)], 0) * (1.0 / math.sqrt(LEAF))

def translations(box_ids, segment_num, phase_scale):
    scale_mod = phase_scale[0] % modulus
    base_key = (box_ids * 37 + 101 * segment_num) % (modulus - 1) + 1
    unit_phase = scale_mod * base_key % modulus
    indices = jnp.arange(WIDTH, dtype=jnp.int32)
    prod_a = (indices[:, None] + 1) * (indices[None, :] + 2) % modulus
    prod_b = (indices[:, None] + 3) * (indices[None, :] + 1) % modulus
    phase_a = prod_a[:, :, None] * unit_phase[None, None, :] % modulus
    phase_b = (prod_b[:, :, None] * unit_phase[None, None, :] + 4096) % modulus
    factor = 2.0 * math.pi / modulus
    ident = jnp.eye(WIDTH, dtype=jnp.float32)[:, :, None]
    own_map = 0.85 * ident + 0.35 / math.sqrt(WIDTH) * jnp.cos(phase_a.astype(jnp.float32) * factor)
    cross_map = 0.6 / math.sqrt(WIDTH) * jnp.cos(phase_b.astype(jnp.float32) * factor)
    return (own_map, cross_map)

def reference(basis_vector, diagonal, coords, phase_scale, sketch_rows, sketch_signs):
    highest = lax.Precision.HIGHEST
    columns = basis_vector.shape[0]
    points = basis_vector.shape[1]
    box_count = points // LEAF
    leaf_map = leaf_table(coords, phase_scale)
    leaf_boxes = leaf_map.reshape(WIDTH, box_count, LEAF)
    blocks = basis_vector.reshape(columns, box_count, LEAF)
    coeffs = jnp.einsum('wbs,qbs->wqb', leaf_boxes, blocks, precision=highest)
    coeffs = coeffs.reshape(WIDTH, columns, N_BOX, BOX_DEV)
    box_ids = jnp.arange(box_count, dtype=jnp.int32)
    for segment_num in range(SECTIONS):
        stride = 2 ** segment_num
        grouped = coeffs.reshape(WIDTH, columns, N_BOX // (2 * stride), 2, stride, BOX_DEV)
        partner = grouped[:, :, :, ::-1].reshape(WIDTH, columns, N_BOX, BOX_DEV)
        own_map, cross_map = translations(box_ids, segment_num, phase_scale)
        own_map = own_map.reshape(WIDTH, WIDTH, N_BOX, BOX_DEV)
        cross_map = cross_map.reshape(WIDTH, WIDTH, N_BOX, BOX_DEV)
        coeffs = jnp.einsum('wvdg,vqdg->wqdg', own_map, coeffs, precision=highest) + jnp.einsum('wvdg,vqdg->wqdg', cross_map, partner, precision=highest)
    target_coef = coeffs.reshape(WIDTH, columns, box_count)
    applied = jnp.einsum('wbs,wqb->qbs', leaf_boxes, target_coef, precision=highest).reshape(columns, points)
    image = diagonal[None, :] * basis_vector + applied
    inner_vw = lax.optimization_barrier(jnp.mean(basis_vector * image, axis=1))
    square = lax.optimization_barrier(jnp.mean(basis_vector * basis_vector, axis=1)) + epsilon
    projection = inner_vw / square
    residual = image - projection[:, None] * basis_vector
    spread = jnp.sqrt(lax.optimization_barrier(jnp.mean(residual * residual, axis=1)) + epsilon)
    new_basis = residual / spread[:, None]
    sign_values = (2 * sketch_signs - 1).astype(jnp.float32)
    signed = new_basis * sign_values[None, :]
    sketch = jnp.zeros((columns, SKETCH), jnp.float32).at[:, sketch_rows].add(signed) * math.sqrt(SKETCH / points)
    arnoldi = jnp.stack([projection, spread])
    return (new_basis, sketch, arnoldi)
```

```python
import functools
import math

import jax
import jax.numpy as jnp
from jax import lax
from jax.experimental import pallas as pl
from jax.experimental.pallas import tpu as pltpu
from jax.sharding import Mesh
from jax.sharding import PartitionSpec as P

RANK = 16
WIDTH = 32
LEAF = 32
SKETCH = 2048
NRHS = 16
SECTIONS = 8
CHIPS = 128
NPTS = 1048576
MOD = 8191
EPS = 1e-06
CHIP = ("box_0", "box_1", "box_2")
CORE = "box_3"
FORWARD = 6
BACK = 9
F32 = jnp.float32


def fold(x):
    return (x & MOD) + (x >> 13)


def unit_circle(phase):
    r = phase.astype(F32)
    r = jnp.where(r > 4095.5, r - float(MOD), r)
    y = r * (math.pi / MOD)
    y2 = y * y
    s = 1.0 / math.factorial(13)
    for k in (11, 9, 7, 5, 3, 1):
        s = s * y2 + (-1.0) ** (k // 2) / math.factorial(k)
    s = s * y
    c = -1.0 / math.factorial(14)
    for k in (12, 10, 8, 6, 4, 2, 0):
        c = c * y2 + (-1.0) ** (k // 2) / math.factorial(k)
    return 1.0 - 2.0 * s * s, 2.0 * s * c


def times(a, b):
    return a[0] * b[0] - a[1] * b[1], a[0] * b[1] + a[1] * b[0]


def pack_kernel(v_ref, coords_ref, diag_ref, rows_ref, signs_ref, out_ref, turned):
    zeros = jnp.zeros((11, 128), F32)
    for jb in range(8):
        tiles = []
        for jt in range(4):
            cols = pl.ds((jb * 4 + jt) * 128, 128)
            tiles += [
                v_ref[:, cols],
                coords_ref[:, cols].astype(F32),
                diag_ref[:, cols],
                rows_ref[:, cols].astype(F32),
                signs_ref[:, cols].astype(F32),
                zeros,
            ]
        turned[pl.ds(jb * 128, 128), :] = jnp.concatenate(tiles, 0).T
    lane = lax.broadcasted_iota(jnp.int32, (32, 128), 1)
    for jt in range(4):
        made = {}
        for s in range(LEAF):
            rows = turned[pl.ds(s, 32, stride=32), :]
            for col, start, width, at in (
                (s // 8, jt * 32, 16, 16 * (s % 8)),
                (4 + s // 16, jt * 32 + 16, 8, 8 * (s % 16)),
            ):
                shift = (at - start) % 128
                moved = pltpu.roll(rows, shift, 1) if shift else rows
                if col in made:
                    moved = jnp.where(lane >= at, moved, made[col])
                made[col] = moved
        for col in range(FORWARD):
            out_ref[pl.ds(jt * 32 * FORWARD + col, 32, stride=FORWARD), :] = made[col]


def product(out_count, terms, store, start=None):
    def tile(t, carry):
        accs = [None] * 8
        if start is not None:
            accs = [start(t * 8 + i) for i in range(8)]
        for matrix, vector in terms:
            for b in range(32):
                vec = vector(b)
                for i in range(8):
                    term = matrix(t * 8 + i, b) * vec
                    accs[i] = term if accs[i] is None else accs[i] + term
        for i in range(8):
            store(t * 8 + i, accs[i])
        return carry

    lax.fori_loop(0, out_count // 8, tile, 0)


def row16(a):
    return pl.ds(pl.multiple_of(a * 16, 16), 16)


def leaf_kernel(info_ref, got_ref, coeffs_ref, leaf_ref, points_ref):
    for c in range(FORWARD):
        points_ref[pl.ds(c * 128, 128), :] = got_ref[pl.ds(c, 128, stride=FORWARD), :].T
    scale = info_ref[0]

    def powers(field):
        where = points_ref[pl.ds(512 + field, 32, stride=8), :].astype(jnp.int32)
        one = unit_circle(fold(fold(where * scale)))
        two = times(one, one)
        return [one, two, times(two, one), times(two, two)]

    first, second = powers(0), powers(1)
    gain = 1.0 / math.sqrt(LEAF)
    second = [(c * gain, s * gain) for c, s in second]
    for w in range(RANK):
        c, s = times(first[w % 4], second[w // 4])
        leaf_ref[w] = c
        leaf_ref[w + RANK] = s

    def store(a, x):
        coeffs_ref[row16(a), :] = x

    product(
        WIDTH,
        [(lambda a, b: leaf_ref[a, b : b + 1, :], lambda b: points_ref[pl.ds(b * 16, 16), :])],
        store,
    )


def section_map(map_ref, unit, offset, first_power, turn, gain):
    index = lax.broadcasted_iota(jnp.int32, (WIDTH, 128), 0) + offset
    one = unit_circle(fold(fold(unit * index)))
    two = times(one, one)
    four = times(two, two)
    scale = (gain * math.cos(turn), gain * math.sin(turn))
    power = one if first_power == 1 else times(two, one)
    power = (
        power[0] * scale[0] - power[1] * scale[1],
        power[0] * scale[1] + power[1] * scale[0],
    )
    fine = [power]
    for _ in range(3):
        fine.append(times(fine[-1], one))
    coarse = None
    for i in range(8):
        for j in range(4):
            c, s = fine[j]
            map_ref[4 * i + j] = c if coarse is None else coarse[0] * c - coarse[1] * s
        coarse = four if coarse is None else times(coarse, four)


def state_rows(parts):
    pad = [jnp.zeros((128 - 16 * len(parts), 128), F32)]
    return jnp.sum(jnp.concatenate(parts + pad, 0).T, axis=0, keepdims=True)


def core_kernel(
    info_ref,
    coeffs_ref,
    partner_ref,
    leaf_ref,
    points_ref,
    out_ref,
    now,
    other,
    later,
    own_map,
    cross_map,
    image,
    high,
    low,
    lhs,
    rhs,
):
    scale, chip, core = info_ref[0], info_ref[1], info_ref[2]
    place = ((chip >> 2) & 7) * 16 + (chip >> 5) * 4 + (chip & 3)
    lane = lax.broadcasted_iota(jnp.int32, (1, 128), 1)
    box = (lane * 2 + core) * 128 + place
    now[...] = coeffs_ref[...]
    other[...] = partner_ref[...]
    lanes = lax.broadcasted_iota(jnp.int32, (NRHS, 128), 1)

    def section(k, carry):
        key = box * 37 + 101 * k
        whole = (key.astype(F32) * (1.0 / (MOD - 1))).astype(jnp.int32)
        key = key - whole * (MOD - 1)
        key = jnp.where(key < 0, key + (MOD - 1), key)
        key = jnp.where(key >= MOD - 1, key - (MOD - 1), key)
        unit = fold(fold((key + 1) * scale))
        section_map(own_map, unit, 2, 1, 0.0, 0.35 / math.sqrt(WIDTH))
        section_map(cross_map, unit, 1, 3, 2.0 * math.pi * 4096 / MOD, 0.6 / math.sqrt(WIDTH))

        def store(a, x):
            later[row16(a), :] = x

        product(
            WIDTH,
            [
                (lambda a, b: own_map[a, b : b + 1, :], lambda b: now[pl.ds(b * 16, 16), :]),
                (lambda a, b: cross_map[a, b : b + 1, :], lambda b: other[pl.ds(b * 16, 16), :]),
            ],
            store,
            lambda a: 0.85 * now[row16(a), :],
        )
        step = jnp.left_shift(1, jnp.minimum(k, SECTIONS - 2))
        bit = (lanes & step) == 0
        for a in range(WIDTH):
            x = later[pl.ds(a * 16, 16), :]
            now[pl.ds(a * 16, 16), :] = x
            other[pl.ds(a * 16, 16), :] = jnp.where(
                bit, pltpu.roll(x, 128 - step, 1), pltpu.roll(x, step, 1)
            )
        return carry

    lax.fori_loop(0, SECTIONS, section, 0)

    rows = points_ref[pl.ds(512 + 3, 32, stride=8), :].astype(jnp.int32)
    high[...] = rows >> 8
    low[...] = rows & 255
    square = jnp.zeros((NRHS, 128), F32)
    inner = jnp.zeros((NRHS, 128), F32)
    for t in range(4):
        accs = [None] * 8
        for w in range(WIDTH):
            vec = now[pl.ds(w * 16, 16), :]
            for i in range(8):
                s = t * 8 + i
                term = leaf_ref[w, s : s + 1, :] * vec
                accs[i] = term if accs[i] is None else accs[i] + term
        for i in range(8):
            s = t * 8 + i
            v = points_ref[pl.ds(s * 16, 16), :]
            x = points_ref[pl.ds(512 + s * 8 + 2, 1), :] * v + accs[i]
            image[pl.ds(s * 16, 16), :] = x
            square += v * v
            inner += v * x
    sums = state_rows([square, inner])
    valid = lane < 16
    vv = jnp.where(valid, sums, 0.0)
    iv = jnp.where(valid, pltpu.roll(sums, 112, 1), 0.0)
    local = jnp.where(vv > 0.0, iv / jnp.where(vv > 0.0, vv, 1.0), 0.0)
    across = jnp.broadcast_to(local, (128, 128)).T[0:NRHS, :]
    energy = jnp.zeros((NRHS, 128), F32)
    mixed = jnp.zeros((NRHS, 128), F32)
    hot = lax.broadcasted_iota(jnp.int32, (256, 128), 0)
    for s in range(LEAF):
        v = points_ref[pl.ds(s * 16, 16), :]
        x = image[pl.ds(s * 16, 16), :]
        r = x - across * v
        energy += r * r
        mixed += r * v
        sign = 2.0 * points_ref[pl.ds(512 + s * 8 + 4, 1), :] - 1.0
        parts = []
        for y in (x * sign, v * sign):
            top = y.astype(jnp.bfloat16).astype(F32)
            parts.append((top, y - top))
        which = high[s : s + 1, :]
        cols = pl.ds(s * 128, 128)
        for h in range(8):
            mask = jnp.broadcast_to(which == h, (NRHS, 128))
            for p in range(2):
                for c in range(2):
                    lhs[pl.ds(p * 256 + h * 32 + c * 16, 16), cols] = jnp.where(
                        mask, parts[c][p], 0.0
                    ).astype(jnp.bfloat16)
        rhs[:, cols] = jnp.where(hot == low[s : s + 1, :], 1.0, 0.0).astype(jnp.bfloat16)
    spread_out = lax.dot_general(
        lhs[...], rhs[...], (((1,), (1,)), ((), ())), preferred_element_type=F32
    )
    spread_out = spread_out[0:256] + spread_out[256:512]
    for c in range(4):
        out_ref[pl.ds(c, 128, stride=BACK), :] = image[pl.ds(c * 128, 128), :].T
    for c in range(2):
        for half in range(2):
            tile = jnp.concatenate(
                [
                    spread_out[
                        (t // 2) * 32 + c * 16 : (t // 2) * 32 + c * 16 + 16,
                        (t % 2) * 128 : (t % 2) * 128 + 128,
                    ]
                    for t in range(half * 8, half * 8 + 8)
                ],
                0,
            )
            out_ref[pl.ds(4 + c * 2 + half, 128, stride=BACK), :] = tile.T
    rest = jnp.where(lane < 32, state_rows([energy, mixed]), 0.0)
    state = vv + pltpu.roll(local, 16, 1) + pltpu.roll(rest, 32, 1)
    out_ref[pl.ds(8, 128, stride=BACK), :] = jnp.broadcast_to(state, (128, 128))


def merged(vv, p, e, cr, total):
    square = total(vv)
    inner = total(p * vv + cr)
    local = jnp.where(square > 0.0, inner / jnp.where(square > 0.0, square, 1.0), 0.0)
    return square, inner, local


def moved_energy(vv, p, e, cr, at, total):
    off = p - at
    return total(e + off * (2.0 * cr + off * vv)), total(cr + off * vv)


def sum_kernel(got_ref, out_ref):
    for c in range(4):
        out_ref[c : c + 1, :] = jnp.sum(
            got_ref[pl.ds(4 + c, 128, stride=BACK), :], axis=0, keepdims=True
        )
    state = got_ref[pl.ds(8, 128, stride=BACK), :]
    valid = lax.broadcasted_iota(jnp.int32, (128, 128), 1) < 16
    parts = [
        jnp.where(valid, pltpu.roll(state, (128 - 16 * i) % 128, 1) if i else state, 0.0)
        for i in range(4)
    ]

    def total(x):
        return jnp.sum(x, axis=0, keepdims=True)

    square, inner, local = merged(*parts, total)
    energy, mixed = moved_energy(*parts, local, total)
    for i, x in enumerate((square, local, energy, mixed)):
        out_ref[4 + i : 5 + i, :] = x


def finish_kernel(got_ref, mine_ref, theirs_ref, v_ref, basis_ref, chunk_ref, arnoldi_ref, turned):
    both = [(mine_ref[4 + i : 5 + i, :], theirs_ref[4 + i : 5 + i, :]) for i in range(4)]
    vv, p, e, cr = both
    square = vv[0] + vv[1]
    inner = (p[0] * vv[0] + cr[0]) + (p[1] * vv[1] + cr[1])
    proj = (inner / NPTS) / (square / NPTS + EPS)
    terms = []
    for i in range(2):
        off = p[i] - proj
        terms.append(e[i] + off * (2.0 * cr[i] + off * vv[i]))
    spread = jnp.sqrt(jnp.maximum(terms[0] + terms[1], 0.0) / NPTS + EPS)
    arnoldi_ref[0:1, :] = proj[:, 0:NRHS]
    arnoldi_ref[1:2, :] = spread[:, 0:NRHS]
    valid = lax.broadcasted_iota(jnp.int32, (1, 128), 1) < 16

    def tiled(x):
        x = jnp.where(valid, x, 0.0)
        for shift in (16, 32, 64):
            x = x + pltpu.roll(x, shift, 1)
        return x

    proj, spread = tiled(proj), tiled(spread)
    sums = mine_ref[0:4, :] + theirs_ref[0:4, :]
    chunk = (sums[0:2] - proj * sums[2:4]) / spread * math.sqrt(SKETCH / NPTS)
    for i in range(2):
        chunk_ref[pl.ds(i, 128, stride=2), :] = jnp.broadcast_to(chunk[i : i + 1], (128, 128))
    proj = jnp.broadcast_to(proj, (128, 128)).T[0:NRHS, :]
    spread = jnp.broadcast_to(spread, (128, 128)).T[0:NRHS, :]
    lane = lax.broadcasted_iota(jnp.int32, (32, 128), 1)
    for s in range(LEAF):
        made = None
        for jt in range(4):
            rows = got_ref[pl.ds(jt * 32 * BACK + s // 8, 32, stride=BACK), :]
            shift = (jt * 32 - (s % 8) * 16) % 128
            rows = pltpu.roll(rows, shift, 1) if shift else rows
            made = rows if made is None else jnp.where(lane >= jt * 32, rows, made)
        turned[pl.ds(s, 32, stride=32), :] = made
    for jb in range(8):
        back = turned[pl.ds(jb * 128, 128), :].T
        for jt in range(4):
            cols = pl.ds((jb * 4 + jt) * 128, 128)
            x = back[jt * 32 : jt * 32 + 16, :]
            basis_ref[:, cols] = (x - proj * v_ref[:, cols]) / spread


def spread_kernel(got_ref, out_ref):
    for half in range(2):
        tile = got_ref[pl.ds(half, 128, stride=2), :].T
        for t in range(8):
            out_ref[:, pl.ds((half * 8 + t) * 128, 128)] = tile[t * 16 : t * 16 + 16, :]


VMEM = pl.BlockSpec(memory_space=pltpu.VMEM)
SMEM = pl.BlockSpec(memory_space=pltpu.SMEM)


def f32(*shape):
    return jax.ShapeDtypeStruct(shape, F32)


def call(kernel, out, ins, scratch=(), flops=1000000):
    single = not isinstance(out, tuple)
    return pl.pallas_call(
        kernel,
        out_shape=out,
        in_specs=ins,
        out_specs=VMEM if single else tuple(VMEM for _ in out),
        scratch_shapes=list(scratch),
        cost_estimate=pl.CostEstimate(flops=flops, bytes_accessed=1000000, transcendentals=0),
        compiler_params=pltpu.CompilerParams(vmem_limit_bytes=48 * 1024 * 1024),
    )


def exchange(x, columns):
    x = lax.all_to_all(x.reshape(CHIPS, columns, 128), CHIP, 0, 0, tiled=True)
    return x.reshape(CHIPS * columns, 128)


def body(basis_vector, diagonal, coords, phase_scale, sketch_rows, sketch_signs):
    chip = lax.axis_index(CHIP)
    core = lax.axis_index(CORE)
    info = jnp.stack([phase_scale[0] % MOD, chip, core]).astype(jnp.int32)
    points = LEAF * CHIPS
    packed = call(pack_kernel, f32(CHIPS * FORWARD, 128), [VMEM] * 5, [pltpu.VMEM((1024, 128), F32)])(
        basis_vector,
        coords,
        diagonal.reshape(1, points),
        sketch_rows.reshape(1, points),
        sketch_signs.reshape(1, points),
    )
    got = exchange(packed, FORWARD)
    coeffs, leaf, held = call(
        leaf_kernel,
        (f32(512, 128), f32(WIDTH, LEAF, 128), f32(FORWARD * 128, 128)),
        [SMEM, VMEM],
    )(info, got)
    partner = lax.ppermute(coeffs, CORE, [(0, 1), (1, 0)])
    big = pltpu.VMEM((512, 128), F32)
    square = pltpu.VMEM((WIDTH, WIDTH, 128), F32)
    index = pltpu.VMEM((LEAF, 128), jnp.int32)
    back = call(
        core_kernel,
        f32(CHIPS * BACK, 128),
        [SMEM] + [VMEM] * 4,
        [
            big,
            big,
            big,
            square,
            square,
            big,
            index,
            index,
            pltpu.VMEM((512, points), jnp.bfloat16),
            pltpu.VMEM((256, points), jnp.bfloat16),
        ],
    )(info, coeffs, partner, leaf, held)
    home = exchange(back, BACK)
    mine = call(sum_kernel, f32(8, 128), [VMEM])(home)
    theirs = lax.ppermute(mine, CORE, [(0, 1), (1, 0)])
    new_basis, chunk, arnoldi = call(
        finish_kernel,
        (f32(NRHS, points), f32(CHIPS * 2, 128), f32(2, NRHS)),
        [VMEM] * 4,
        [pltpu.VMEM((1024, 128), F32)],
    )(home, mine, theirs, basis_vector)
    sketch = call(spread_kernel, f32(NRHS, SKETCH), [VMEM])(exchange(chunk, 2))
    return new_basis, sketch, arnoldi


def solution(mesh):
    torus = Mesh(mesh.devices.reshape(4, 8, 4, 2), ("box_0", "box_1", "box_2", "box_3"))
    box = ("box_0", "box_1", "box_2", "box_3")
    placed = (P(None, box), P(box), P(None, box), P(), P(box), P(box))
    return jax.shard_map(
        body, mesh=torus, in_specs=placed, out_specs=(P(None, box), P(), P()), check_vma=False
    )
```

```python
import functools
import math

import jax
import jax.numpy as jnp
from jax import lax
from jax.experimental import pallas as pl
from jax.experimental.pallas import tpu as pltpu
from jax.sharding import Mesh
from jax.sharding import PartitionSpec as P

RANK = 16
WIDTH = 32
LEAF = 32
SKETCH = 2048
NRHS = 16
SECTIONS = 8
CHIPS = 128
NPTS = 1048576
MOD = 8191
EPS = 1e-06
CHIP = ("box_0", "box_1", "box_2")
CORE = "box_3"
OUT_ROWS = 6
BACK_ROWS = 9
EARLY_MIB = 24
CORE_MIB = 47
F32 = jnp.float32


def fold(x):
    return (x & MOD) + (x >> 13)


def unit_circle(phase):
    r = phase.astype(F32)
    r = jnp.where(r > 4095.5, r - float(MOD), r)
    y = r * (math.pi / MOD)
    y2 = y * y
    s = 1.0 / math.factorial(13)
    for k in (11, 9, 7, 5, 3, 1):
        s = s * y2 + (-1.0) ** (k // 2) / math.factorial(k)
    s = s * y
    c = -1.0 / math.factorial(14)
    for k in (12, 10, 8, 6, 4, 2, 0):
        c = c * y2 + (-1.0) ** (k // 2) / math.factorial(k)
    return 1.0 - 2.0 * s * s, 2.0 * s * c


def times(a, b):
    return a[0] * b[0] - a[1] * b[1], a[0] * b[1] + a[1] * b[0]


def split_rows(lhs, y, high, cols):
    top = y.astype(jnp.bfloat16).astype(F32)
    for p, part in enumerate((top, y - top)):
        for h in range(8):
            mask = jnp.broadcast_to(high == h, (NRHS, 128))
            lhs[pl.ds(p * 128 + h * 16, 16), cols] = jnp.where(mask, part, 0.0).astype(jnp.bfloat16)


def hot_rows(rhs, low, cols):
    index = lax.broadcasted_iota(jnp.int32, (256, 128), 0)
    rhs[:, cols] = jnp.where(index == low, 1.0, 0.0).astype(jnp.bfloat16)


def sketched(lhs, rhs, out_ref, at, stride):
    both = lax.dot_general(
        lhs[...], rhs[...], (((1,), (1,)), ((), ())), preferred_element_type=F32
    )
    both = both[0:128] + both[128:256]
    for half in range(2):
        tile = jnp.concatenate(
            [
                both[(t // 2) * 16 : (t // 2) * 16 + 16, (t % 2) * 128 : (t % 2) * 128 + 128]
                for t in range(half * 8, half * 8 + 8)
            ],
            0,
        )
        out_ref[pl.ds(at + half, 128, stride=stride), :] = tile.T


def fetch(sources, held, sems):
    copies = [pltpu.make_async_copy(a, b, sems.at[i]) for i, (a, b) in enumerate(zip(sources, held))]
    for copy in copies:
        copy.start()
    for copy in copies:
        copy.wait()


def pack_kernel(*refs):
    sources, out_ref, held, turned, sems = refs[:5], refs[5], refs[6:11], refs[11], refs[12]
    fetch(sources, held, sems)
    v_ref, coords_ref, diag_ref, rows_ref, signs_ref = held
    zeros = jnp.zeros((11, 128), F32)
    for jb in range(8):
        tiles = []
        for jt in range(4):
            j = jb * 4 + jt
            cols = pl.ds(j * 128, 128)
            tiles += [
                v_ref[:, cols],
                coords_ref[:, cols].astype(F32),
                diag_ref[j : j + 1, :],
                rows_ref[j : j + 1, :].astype(F32),
                signs_ref[j : j + 1, :].astype(F32),
                zeros,
            ]
        turned[pl.ds(jb * 128, 128), :] = jnp.concatenate(tiles, 0).T
    lane = lax.broadcasted_iota(jnp.int32, (32, 128), 1)
    for jt in range(4):
        made = {}
        for s in range(LEAF):
            rows = turned[pl.ds(s, 32, stride=32), :]
            for col, start, at in (
                (s // 8, jt * 32, 16 * (s % 8)),
                (4 + s // 16, jt * 32 + 16, 8 * (s % 16)),
            ):
                shift = (at - start) % 128
                moved = pltpu.roll(rows, shift, 1) if shift else rows
                if col in made:
                    moved = jnp.where(lane >= at, moved, made[col])
                made[col] = moved
        for col, rows in made.items():
            out_ref[pl.ds(jt * 32 * OUT_ROWS + col, 32, stride=OUT_ROWS), :] = rows


def product(out_count, terms, store, start=None, width=16, group=8):
    def tile(t, carry):
        accs = [jnp.zeros((8, 128), F32)] * (2 * width)
        if start is not None:
            accs = [x for i in range(width) for x in start(t * width + i)]

        def some(g, accs):
            accs = list(accs)
            for matrix, vector in terms:
                for i in range(group):
                    b = g * group + i
                    vec = vector(b)
                    for i in range(width):
                        row = jnp.broadcast_to(matrix(t * width + i, b), (8, 128))
                        for half in range(2):
                            accs[2 * i + half] += row * vec[half]
            return tuple(accs)

        accs = lax.fori_loop(0, 32 // group, some, tuple(accs))
        for i in range(width):
            store(t * width + i, accs[2 * i : 2 * i + 2])
        return carry

    lax.fori_loop(0, out_count // width, tile, 0)


def halves(ref, a, *lead):
    return [ref[(*lead, pl.ds(pl.multiple_of(a * 16 + 8 * h, 8), 8), slice(None))] for h in range(2)]


def row16(a):
    return pl.ds(pl.multiple_of(a * 16, 16), 16)


def leaf_kernel(info_ref, got_ref, after_ref, coeffs_ref, leaf_ref, points_ref):
    for c in range(6):
        points_ref[pl.ds(c * 128, 128), :] = got_ref[pl.ds(c, 128, stride=OUT_ROWS), :].T
    scale = info_ref[0]

    def powers(field):
        where = points_ref[pl.ds(512 + field, 32, stride=8), :].astype(jnp.int32)
        one = unit_circle(fold(fold(where * scale)))
        two = times(one, one)
        return [one, two, times(two, one), times(two, two)]

    first, second = powers(0), powers(1)
    gain = 1.0 / math.sqrt(LEAF)
    second = [(c * gain, s * gain) for c, s in second]
    for w in range(RANK):
        c, s = times(first[w % 4], second[w // 4])
        leaf_ref[w] = c
        leaf_ref[w + RANK] = s

    def store(a, x):
        coeffs_ref[row16(a), :] = jnp.concatenate(x, 0)

    product(
        WIDTH,
        [(lambda a, b: leaf_ref[a, pl.ds(b, 1), :], lambda b: halves(points_ref, b))],
        store,
    )


def section_map(map_ref, unit, offset, first_power, turn, gain):
    index = lax.broadcasted_iota(jnp.int32, (WIDTH, 128), 0) + offset
    one = unit_circle(fold(fold(unit * index)))
    two = times(one, one)
    four = times(two, two)
    scale = (gain * math.cos(turn), gain * math.sin(turn))
    power = one if first_power == 1 else times(two, one)
    power = (
        power[0] * scale[0] - power[1] * scale[1],
        power[0] * scale[1] + power[1] * scale[0],
    )
    fine = [power]
    for _ in range(3):
        fine.append(times(fine[-1], one))
    coarse = None
    for i in range(8):
        for j in range(4):
            c, s = fine[j]
            map_ref[4 * i + j] = c if coarse is None else coarse[0] * c - coarse[1] * s
        coarse = four if coarse is None else times(coarse, four)


def state_rows(parts):
    pad = [jnp.zeros((128 - 16 * len(parts), 128), F32)]
    return jnp.sum(jnp.concatenate(parts + pad, 0).T, axis=0, keepdims=True)


def section_maps(info_ref, k, maps_ref):
    scale, chip, core = info_ref[0], info_ref[1], info_ref[2]
    place = ((chip >> 2) & 7) * 16 + (chip >> 5) * 4 + (chip & 3)
    lane = lax.broadcasted_iota(jnp.int32, (1, 128), 1)
    key = ((lane * 2 + core) * 128 + place) * 37 + 101 * k
    whole = (key.astype(F32) * (1.0 / (MOD - 1))).astype(jnp.int32)
    key = key - whole * (MOD - 1)
    key = jnp.where(key < 0, key + (MOD - 1), key)
    key = jnp.where(key >= MOD - 1, key - (MOD - 1), key)
    unit = fold(fold((key + 1) * scale))
    turn = 2.0 * math.pi * 4096 / MOD
    section_map(maps_ref.at[0], unit, 2, 1, 0.0, 0.35 / math.sqrt(WIDTH))
    section_map(maps_ref.at[1], unit, 1, 3, turn, 0.6 / math.sqrt(WIDTH))


def early_kernel(info_ref, *refs):
    sources, maps_ref, sketch_ref, done_ref = refs[:3], *refs[3:6]
    held, lhs, rhs, sems = refs[6:9], *refs[9:]
    fetch(sources, held, sems)
    v_ref, rows_ref, signs_ref = held

    def section(k, carry):
        section_maps(info_ref, k, maps_ref.at[k - 1])
        return carry

    lax.fori_loop(1, SECTIONS, section, 0)
    for j in range(32):
        cols = pl.ds(j * 128, 128)
        rows, signs = rows_ref[j : j + 1, :], signs_ref[j : j + 1, :]
        split_rows(lhs, v_ref[:, cols] * (2 * signs - 1).astype(F32), rows >> 8, cols)
        hot_rows(rhs, rows & 255, cols)
    sketched(lhs, rhs, sketch_ref, 0, 2)
    done_ref[...] = jnp.zeros((8, 128), F32)


def hot_kernel(info_ref, points_ref, rhs_ref, maps_ref):
    for s in range(LEAF):
        low = points_ref[pl.ds(512 + s * 8 + 3, 1), :].astype(jnp.int32) & 255
        hot_rows(rhs_ref, low, pl.ds(s * 128, 128))
    section_maps(info_ref, 0, maps_ref)


def core_kernel(
    coeffs_ref,
    partner_ref,
    leaf_ref,
    points_ref,
    first,
    rhs,
    vsketch_ref,
    maps_hbm,
    out_ref,
    now,
    other,
    image,
    lhs,
    maps,
    sems,
):
    lane = lax.broadcasted_iota(jnp.int32, (1, 128), 1)
    lanes = lax.broadcasted_iota(jnp.int32, (NRHS, 128), 1)

    def copy(k):
        return pltpu.make_async_copy(maps_hbm.at[k - 1], maps.at[k & 1], sems.at[k & 1])

    copy(1).start()
    now[0] = coeffs_ref[...]
    other[0] = partner_ref[...]

    def section(k, own, cross):
        at = k & 1
        step = jnp.left_shift(1, jnp.minimum(k, SECTIONS - 2))
        bit = (lanes & step) == 0

        def store(a, x):
            x = jnp.concatenate(x, 0)
            now[1 - at, row16(a), :] = x
            other[1 - at, row16(a), :] = jnp.where(
                bit, pltpu.roll(x, 128 - step, 1), pltpu.roll(x, step, 1)
            )

        product(
            WIDTH,
            [
                (lambda a, b: own[a, pl.ds(b, 1), :], lambda b: halves(now, b, at)),
                (lambda a, b: cross[a, pl.ds(b, 1), :], lambda b: halves(other, b, at)),
            ],
            store,
            lambda a: [0.85 * x for x in jnp.split(now[at, row16(a), :], 2)],
        )

    section(jnp.int32(0), first.at[0], first.at[1])

    def later(k, carry):
        copy(k).wait()

        @pl.when(k < SECTIONS - 1)
        def _():
            copy(k + 1).start()

        section(k, maps.at[k & 1, 0], maps.at[k & 1, 1])
        return carry

    lax.fori_loop(1, SECTIONS, later, 0)

    square = jnp.zeros((NRHS, 128), F32)
    inner = jnp.zeros((NRHS, 128), F32)
    for t in range(2):
        accs = [None] * 16
        for w in range(WIDTH):
            vec = now[0, pl.ds(w * 16, 16), :]
            for i in range(16):
                s = t * 16 + i
                term = leaf_ref[w, s : s + 1, :] * vec
                accs[i] = term if accs[i] is None else accs[i] + term
        for i in range(16):
            s = t * 16 + i
            v = points_ref[pl.ds(s * 16, 16), :]
            x = points_ref[pl.ds(512 + s * 8 + 2, 1), :] * v + accs[i]
            image[pl.ds(s * 16, 16), :] = x
            square += v * v
            inner += v * x
            sign = 2.0 * points_ref[pl.ds(512 + s * 8 + 4, 1), :] - 1.0
            high = points_ref[pl.ds(512 + s * 8 + 3, 1), :].astype(jnp.int32) >> 8
            split_rows(lhs, x * sign, high, pl.ds(s * 128, 128))
    sums = state_rows([square, inner])
    valid = lane < 16
    vv = jnp.where(valid, sums, 0.0)
    iv = jnp.where(valid, pltpu.roll(sums, 112, 1), 0.0)
    local = jnp.where(vv > 0.0, iv / jnp.where(vv > 0.0, vv, 1.0), 0.0)
    across = jnp.broadcast_to(local, (128, 128)).T[0:NRHS, :]
    energy = jnp.zeros((NRHS, 128), F32)
    mixed = jnp.zeros((NRHS, 128), F32)
    for s in range(LEAF):
        v = points_ref[pl.ds(s * 16, 16), :]
        r = image[pl.ds(s * 16, 16), :] - across * v
        energy += r * r
        mixed += r * v
    for c in range(4):
        out_ref[pl.ds(c, 128, stride=BACK_ROWS), :] = image[pl.ds(c * 128, 128), :].T
    for c in range(2):
        out_ref[pl.ds(6 + c, 128, stride=BACK_ROWS), :] = vsketch_ref[pl.ds(c, 128, stride=2), :]
    sketched(lhs, rhs, out_ref, 4, BACK_ROWS)
    rest = jnp.where(lane < 32, state_rows([energy, mixed]), 0.0)
    state = vv + pltpu.roll(local, 16, 1) + pltpu.roll(rest, 32, 1)
    out_ref[pl.ds(8, 128, stride=BACK_ROWS), :] = jnp.broadcast_to(state, (128, 128))


def merged(vv, p, e, cr, total):
    square = total(vv)
    inner = total(p * vv + cr)
    local = jnp.where(square > 0.0, inner / jnp.where(square > 0.0, square, 1.0), 0.0)
    return square, inner, local


def moved_energy(vv, p, e, cr, at, total):
    off = p - at
    return total(e + off * (2.0 * cr + off * vv)), total(cr + off * vv)


def sum_kernel(got_ref, out_ref):
    for c in range(4):
        out_ref[c : c + 1, :] = jnp.sum(
            got_ref[pl.ds(4 + c, 128, stride=BACK_ROWS), :], axis=0, keepdims=True
        )
    state = got_ref[pl.ds(8, 128, stride=BACK_ROWS), :]
    valid = lax.broadcasted_iota(jnp.int32, (128, 128), 1) < 16
    parts = [
        jnp.where(valid, pltpu.roll(state, (128 - 16 * i) % 128, 1) if i else state, 0.0)
        for i in range(4)
    ]

    def total(x):
        return jnp.sum(x, axis=0, keepdims=True)

    square, inner, local = merged(*parts, total)
    energy, mixed = moved_energy(*parts, local, total)
    for i, x in enumerate((square, local, energy, mixed)):
        out_ref[4 + i : 5 + i, :] = x


def chunk_kernel(mine_ref, theirs_ref, chunk_ref, arnoldi_ref, scalars_ref):
    both = [(mine_ref[4 + i : 5 + i, :], theirs_ref[4 + i : 5 + i, :]) for i in range(4)]
    vv, p, e, cr = both
    square = vv[0] + vv[1]
    inner = (p[0] * vv[0] + cr[0]) + (p[1] * vv[1] + cr[1])
    proj = (inner / NPTS) / (square / NPTS + EPS)
    terms = []
    for i in range(2):
        off = p[i] - proj
        terms.append(e[i] + off * (2.0 * cr[i] + off * vv[i]))
    spread = jnp.sqrt(jnp.maximum(terms[0] + terms[1], 0.0) / NPTS + EPS)
    arnoldi_ref[0:1, :] = proj[:, 0:NRHS]
    arnoldi_ref[1:2, :] = spread[:, 0:NRHS]
    valid = lax.broadcasted_iota(jnp.int32, (1, 128), 1) < 16

    def tiled(x):
        x = jnp.where(valid, x, 0.0)
        for shift in (16, 32, 64):
            x = x + pltpu.roll(x, shift, 1)
        return x

    proj, spread = tiled(proj), tiled(spread)
    scalars_ref[0:1, :] = proj
    scalars_ref[1:2, :] = spread
    sums = mine_ref[0:4, :] + theirs_ref[0:4, :]
    chunk = (sums[0:2] - proj * sums[2:4]) / spread * math.sqrt(SKETCH / NPTS)
    for i in range(2):
        chunk_ref[pl.ds(i, 128, stride=2), :] = jnp.broadcast_to(chunk[i : i + 1], (128, 128))


def basis_kernel(got_ref, scalars_ref, v_ref, basis_ref, turned):
    proj = jnp.broadcast_to(scalars_ref[0:1, :], (128, 128)).T[0:NRHS, :]
    spread = jnp.broadcast_to(scalars_ref[1:2, :], (128, 128)).T[0:NRHS, :]
    lane = lax.broadcasted_iota(jnp.int32, (32, 128), 1)
    for s in range(LEAF):
        made = None
        for jt in range(4):
            rows = got_ref[pl.ds(jt * 32 * BACK_ROWS + s // 8, 32, stride=BACK_ROWS), :]
            shift = (jt * 32 - (s % 8) * 16) % 128
            rows = pltpu.roll(rows, shift, 1) if shift else rows
            made = rows if made is None else jnp.where(lane >= jt * 32, rows, made)
        turned[pl.ds(s, 32, stride=32), :] = made
    for jb in range(8):
        back = turned[pl.ds(jb * 128, 128), :].T
        for jt in range(4):
            cols = pl.ds((jb * 4 + jt) * 128, 128)
            x = back[jt * 32 : jt * 32 + 16, :]
            basis_ref[:, cols] = (x - proj * v_ref[:, cols]) / spread


def spread_kernel(got_ref, out_ref):
    for half in range(2):
        tile = got_ref[pl.ds(half, 128, stride=2), :].T
        for t in range(8):
            out_ref[:, pl.ds((half * 8 + t) * 128, 128)] = tile[t * 16 : t * 16 + 16, :]


VMEM = pl.BlockSpec(memory_space=pltpu.VMEM)
SMEM = pl.BlockSpec(memory_space=pltpu.SMEM)
HBM = pl.BlockSpec(memory_space=pltpu.HBM)


def f32(*shape):
    return jax.ShapeDtypeStruct(shape, F32)


def call(kernel, out, ins, scratch=(), flops=1000000, mib=12):
    single = not isinstance(out, tuple)
    return pl.pallas_call(
        kernel,
        out_shape=out,
        in_specs=ins,
        out_specs=VMEM if single else tuple(VMEM for _ in out),
        scratch_shapes=list(scratch),
        cost_estimate=pl.CostEstimate(flops=flops, bytes_accessed=1000000, transcendentals=0),
        compiler_params=pltpu.CompilerParams(vmem_limit_bytes=mib * 1024 * 1024),
    )


def exchange(x):
    return lax.all_to_all(x[:, None, :], CHIP, 0, 0, tiled=True)[:, 0, :]


def body(basis_vector, diagonal, coords, phase_scale, sketch_rows, sketch_signs):
    chip = lax.axis_index(CHIP)
    core = lax.axis_index(CORE)
    info = jnp.stack([phase_scale[0] % MOD, chip, core]).astype(jnp.int32)
    points = LEAF * CHIPS
    swap = [(0, 1), (1, 0)]
    sketch_rows, sketch_signs = sketch_rows.reshape(32, 128), sketch_signs.reshape(32, 128)
    vector = pltpu.VMEM((NRHS, points), F32)
    ints = pltpu.VMEM((32, 128), jnp.int32)
    turned = pltpu.VMEM((1024, 128), F32)
    parts = pltpu.VMEM((256, points), jnp.bfloat16)
    hot_type = jax.ShapeDtypeStruct((256, points), jnp.bfloat16)
    packed = call(
        pack_kernel,
        f32(CHIPS * OUT_ROWS, 128),
        [HBM] * 5,
        [
            vector,
            pltpu.VMEM((2, points), jnp.int32),
            pltpu.VMEM((32, 128), F32),
            ints,
            ints,
            turned,
            pltpu.SemaphoreType.DMA((5,)),
        ],
        mib=60,
    )(basis_vector, coords, diagonal.reshape(32, 128), sketch_rows, sketch_signs)
    maps, vsketch, done = call(
        early_kernel,
        (f32(SECTIONS - 1, 2, WIDTH, WIDTH, 128), f32(CHIPS * 2, 128), f32(8, 128)),
        [SMEM] + [HBM] * 3,
        [vector, ints, ints, parts, parts, pltpu.SemaphoreType.DMA((3,))],
        flops=20000000,
        mib=EARLY_MIB,
    )(info, basis_vector, sketch_rows, sketch_signs)
    got = exchange(packed)
    coeffs, leaf, held = call(
        leaf_kernel,
        (f32(512, 128), f32(WIDTH, LEAF, 128), f32(OUT_ROWS * 128, 128)),
        [SMEM, VMEM, HBM],
    )(info, got, done)
    partner = lax.ppermute(coeffs, CORE, swap)
    first_type = f32(2, WIDTH, WIDTH, 128)
    hot, first = call(hot_kernel, (hot_type, first_type), [SMEM, VMEM])(info, held)
    pair = pltpu.VMEM((2, 512, 128), F32)
    back = call(
        core_kernel,
        f32(CHIPS * BACK_ROWS, 128),
        [VMEM] * 7 + [HBM],
        [
            pair,
            pair,
            pltpu.VMEM((512, 128), F32),
            parts,
            pltpu.VMEM((2, 2, WIDTH, WIDTH, 128), F32),
            pltpu.SemaphoreType.DMA((2,)),
        ],
        mib=CORE_MIB,
    )(coeffs, partner, leaf, held, first, hot, vsketch, maps)
    home = exchange(back)
    mine = call(sum_kernel, f32(8, 128), [VMEM])(home)
    theirs = lax.ppermute(mine, CORE, swap)
    chunk, arnoldi, scalars = call(
        chunk_kernel, (f32(CHIPS * 2, 128), f32(2, NRHS), f32(2, 128)), [VMEM] * 2
    )(mine, theirs)
    spread = exchange(chunk)
    new_basis = call(basis_kernel, f32(NRHS, points), [VMEM] * 3, [turned], flops=20000000)(
        home, scalars, basis_vector
    )
    sketch = call(spread_kernel, f32(NRHS, SKETCH), [VMEM])(spread)
    return new_basis, sketch, arnoldi


def solution(mesh):
    torus = Mesh(mesh.devices.reshape(4, 8, 4, 2), ("box_0", "box_1", "box_2", "box_3"))
    box = ("box_0", "box_1", "box_2", "box_3")
    placed = (P(None, box), P(box), P(None, box), P(), P(box), P(box))
    return jax.shard_map(
        body, mesh=torus, in_specs=placed, out_specs=(P(None, box), P(), P()), check_vma=False
    )
```

```python
import functools
import math

import jax
import jax.numpy as jnp
from jax import lax
from jax.experimental import pallas as pl
from jax.experimental.pallas import tpu as pltpu
from jax.sharding import Mesh
from jax.sharding import PartitionSpec as P

RANK = 16
WIDTH = 32
LEAF = 32
SKETCH = 2048
NRHS = 16
SECTIONS = 8
CHIPS = 128
NPTS = 1048576
MOD = 8191
EPS = 1e-06
CHIP = ("box_0", "box_1", "box_2")
CORE = "box_3"
OUT_ROWS = 6
SUM_ROWS = 4
BACK_ROWS = 6
EARLY_MIB = 48
CORE_MIB = 47
F32 = jnp.float32


def fold(x):
    return (x & MOD) + (x >> 13)


def unit_circle(phase):
    r = phase.astype(F32)
    r = jnp.where(r > 4095.5, r - float(MOD), r)
    y = r * (math.pi / MOD)
    y2 = y * y
    s = 1.0 / math.factorial(13)
    for k in (11, 9, 7, 5, 3, 1):
        s = s * y2 + (-1.0) ** (k // 2) / math.factorial(k)
    s = s * y
    c = -1.0 / math.factorial(14)
    for k in (12, 10, 8, 6, 4, 2, 0):
        c = c * y2 + (-1.0) ** (k // 2) / math.factorial(k)
    return 1.0 - 2.0 * s * s, 2.0 * s * c


def times(a, b):
    return a[0] * b[0] - a[1] * b[1], a[0] * b[1] + a[1] * b[0]


def split_rows(lhs, y, high, cols):
    top = y.astype(jnp.bfloat16).astype(F32)
    for p, part in enumerate((top, y - top)):
        for h in range(8):
            mask = jnp.broadcast_to(high == h, (NRHS, 128))
            lhs[pl.ds(p * 128 + h * 16, 16), cols] = jnp.where(mask, part, 0.0).astype(jnp.bfloat16)


def hot_rows(rhs, low, cols):
    index = lax.broadcasted_iota(jnp.int32, (256, 128), 0)
    rhs[:, cols] = jnp.where(index == low, 1.0, 0.0).astype(jnp.bfloat16)


def sketched(lhs, rhs):
    both = lax.dot_general(
        lhs[...], rhs[...], (((1,), (1,)), ((), ())), preferred_element_type=F32
    )
    both = both[0:128] + both[128:256]
    return [
        jnp.concatenate(
            [
                both[(t // 2) * 16 : (t // 2) * 16 + 16, (t % 2) * 128 : (t % 2) * 128 + 128]
                for t in range(half * 8, half * 8 + 8)
            ],
            0,
        ).T
        for half in range(2)
    ]


def fetches(sources, held, sems):
    return [pltpu.make_async_copy(a, b, sems.at[i]) for i, (a, b) in enumerate(zip(sources, held))]


def pack_kernel(*refs):
    sources, out_ref, held, turned, sems = refs[:5], refs[5], refs[6:11], refs[11], refs[12]
    copies = fetches(sources, held, sems)
    for copy in copies:
        copy.start()
    for copy in copies:
        copy.wait()
    v_ref, coords_ref, diag_ref, rows_ref, signs_ref = held
    zeros = jnp.zeros((11, 128), F32)
    for jb in range(8):
        tiles = []
        for jt in range(4):
            j = jb * 4 + jt
            cols = pl.ds(j * 128, 128)
            tiles += [
                v_ref[:, cols],
                coords_ref[:, cols].astype(F32),
                diag_ref[j : j + 1, :],
                rows_ref[j : j + 1, :].astype(F32),
                signs_ref[j : j + 1, :].astype(F32),
                zeros,
            ]
        turned[pl.ds(jb * 128, 128), :] = jnp.concatenate(tiles, 0).T
    lane = lax.broadcasted_iota(jnp.int32, (32, 128), 1)
    made = {}
    for s in range(LEAF):
        rows = turned[pl.ds(s, 32, stride=32), :]
        for col, start, width, at in (
            (s // 8, 0, 16, 16 * (s % 8)),
            (4 + s // 16, 16, 8, 8 * (s % 16)),
        ):
            moved = pltpu.roll(rows, at, 1) if at else rows
            for jt in range(4):
                first = (jt * 32 + start + at) % 128
                if (col, jt) in made:
                    moved_here = jnp.where((lane & -width) == first, moved, made[col, jt])
                else:
                    moved_here = moved
                made[col, jt] = moved_here
    for (col, jt), rows in made.items():
        shift = (-jt * 32 - (16 if col >= 4 else 0)) % 128
        rows = pltpu.roll(rows, shift, 1) if shift else rows
        out_ref[pl.ds(jt * 32 * OUT_ROWS + col, 32, stride=OUT_ROWS), :] = rows


def product(out_count, terms, store, start=None, width=16, group=8):
    def tile(t, carry):
        accs = [jnp.zeros((8, 128), F32)] * (2 * width)
        if start is not None:
            accs = [x for i in range(width) for x in start(t * width + i)]

        def some(g, accs):
            accs = list(accs)
            for matrix, vector in terms:
                for i in range(group):
                    b = g * group + i
                    vec = vector(b)
                    for i in range(width):
                        row = jnp.broadcast_to(matrix(t * width + i, b), (8, 128))
                        for half in range(2):
                            accs[2 * i + half] += row * vec[half]
            return tuple(accs)

        accs = lax.fori_loop(0, 32 // group, some, tuple(accs))
        for i in range(width):
            store(t * width + i, accs[2 * i : 2 * i + 2])
        return carry

    lax.fori_loop(0, out_count // width, tile, 0)


def halves(ref, a, *lead):
    return [ref[(*lead, pl.ds(pl.multiple_of(a * 16 + 8 * h, 8), 8), slice(None))] for h in range(2)]


def row16(a):
    return pl.ds(pl.multiple_of(a * 16, 16), 16)


def leaf_kernel(info_ref, got_ref, after_ref, coeffs_ref, leaf_ref, points_ref):
    for c in range(6):
        points_ref[pl.ds(c * 128, 128), :] = got_ref[pl.ds(c, 128, stride=OUT_ROWS), :].T
    scale = info_ref[0:1, :]

    def powers(field):
        where = points_ref[pl.ds(512 + field, 32, stride=8), :].astype(jnp.int32)
        one = unit_circle(fold(fold(where * scale)))
        two = times(one, one)
        return [one, two, times(two, one), times(two, two)]

    first, second = powers(0), powers(1)
    gain = 1.0 / math.sqrt(LEAF)
    second = [(c * gain, s * gain) for c, s in second]
    for w in range(RANK):
        c, s = times(first[w % 4], second[w // 4])
        leaf_ref[w] = c
        leaf_ref[w + RANK] = s

    def store(a, x):
        coeffs_ref[row16(a), :] = jnp.concatenate(x, 0)

    product(
        WIDTH,
        [(lambda a, b: leaf_ref[a, pl.ds(b, 1), :], lambda b: halves(points_ref, b))],
        store,
    )


def section_map(map_ref, unit, offset, first_power, turn, gain):
    index = lax.broadcasted_iota(jnp.int32, (WIDTH, 128), 0) + offset
    one = unit_circle(fold(fold(unit * index)))
    two = times(one, one)
    four = times(two, two)
    scale = (gain * math.cos(turn), gain * math.sin(turn))
    power = one if first_power == 1 else times(two, one)
    power = (
        power[0] * scale[0] - power[1] * scale[1],
        power[0] * scale[1] + power[1] * scale[0],
    )
    fine = [power]
    for _ in range(3):
        fine.append(times(fine[-1], one))
    coarse = None
    for i in range(8):
        for j in range(4):
            c, s = fine[j]
            map_ref[4 * i + j] = c if coarse is None else coarse[0] * c - coarse[1] * s
        coarse = four if coarse is None else times(coarse, four)


def state_rows(parts):
    pad = [jnp.zeros((128 - 16 * len(parts), 128), F32)]
    return jnp.sum(jnp.concatenate(parts + pad, 0).T, axis=0, keepdims=True)


def section_maps(info_ref, k, maps_ref):
    scale, chip, core = info_ref[0:1, :], info_ref[1:2, :], info_ref[2:3, :]
    place = ((chip >> 2) & 7) * 16 + (chip >> 5) * 4 + (chip & 3)
    lane = lax.broadcasted_iota(jnp.int32, (1, 128), 1)
    key = ((lane * 2 + core) * 128 + place) * 37 + 101 * k
    whole = (key.astype(F32) * (1.0 / (MOD - 1))).astype(jnp.int32)
    key = key - whole * (MOD - 1)
    key = jnp.where(key < 0, key + (MOD - 1), key)
    key = jnp.where(key >= MOD - 1, key - (MOD - 1), key)
    unit = fold(fold((key + 1) * scale))
    turn = 2.0 * math.pi * 4096 / MOD
    section_map(maps_ref.at[0], unit, 2, 1, 0.0, 0.35 / math.sqrt(WIDTH))
    section_map(maps_ref.at[1], unit, 1, 3, turn, 0.6 / math.sqrt(WIDTH))


def early_kernel(info_ref, *refs):
    sources, maps_hbm, keep_ref, give_ref = refs[:3], *refs[3:6]
    held, maps, lhs, rhs, sems, map_sems = refs[6:9], *refs[9:]
    copies = fetches(sources, held, sems)
    for copy in copies:
        copy.start()

    def leave(k):
        return pltpu.make_async_copy(maps.at[k & 1], maps_hbm.at[k - 1], map_sems.at[k & 1])

    def section(k, carry):
        @pl.when(k > 2)
        def _():
            leave(k - 2).wait()

        section_maps(info_ref, k, maps.at[k & 1])
        leave(k).start()
        return carry

    lax.fori_loop(1, SECTIONS, section, 0)
    for copy in copies:
        copy.wait()
    v_ref, rows_ref, signs_ref = held
    for j in range(32):
        cols = pl.ds(j * 128, 128)
        rows, signs = rows_ref[j : j + 1, :], signs_ref[j : j + 1, :]
        split_rows(lhs, v_ref[:, cols] * (2 * signs - 1).astype(F32), rows >> 8, cols)
        hot_rows(rhs, rows & 255, cols)
    low, high = sketched(lhs, rhs)
    first = info_ref[2:3, :] == 0
    first = jnp.broadcast_to(first, (128, 128))
    keep_ref[...] = jnp.where(first, low, high)
    give_ref[...] = jnp.where(first, high, low)
    for k in (SECTIONS - 2, SECTIONS - 1):
        leave(k).wait()


def hot_kernel(info_ref, points_ref, rhs_ref, maps_ref):
    for s in range(LEAF):
        low = points_ref[pl.ds(512 + s * 8 + 3, 1), :].astype(jnp.int32) & 255
        hot_rows(rhs_ref, low, pl.ds(s * 128, 128))
    section_maps(info_ref, 0, maps_ref)


def core_kernel(
    coeffs_ref,
    partner_ref,
    leaf_ref,
    points_ref,
    first,
    rhs,
    keep_ref,
    taken_ref,
    maps_hbm,
    out_ref,
    image_ref,
    now,
    other,
    image,
    lhs,
    maps,
    sems,
):
    lane = lax.broadcasted_iota(jnp.int32, (1, 128), 1)
    lanes = lax.broadcasted_iota(jnp.int32, (NRHS, 128), 1)

    def copy(k):
        return pltpu.make_async_copy(maps_hbm.at[k - 1], maps.at[k & 1], sems.at[k & 1])

    copy(1).start()
    now[0] = coeffs_ref[...]
    other[0] = partner_ref[...]

    def section(k, own, cross):
        at = k & 1
        step = jnp.left_shift(1, jnp.minimum(k, SECTIONS - 2))
        bit = (lanes & step) == 0

        def store(a, x):
            x = jnp.concatenate(x, 0)
            now[1 - at, row16(a), :] = x
            other[1 - at, row16(a), :] = jnp.where(
                bit, pltpu.roll(x, 128 - step, 1), pltpu.roll(x, step, 1)
            )

        product(
            WIDTH,
            [
                (lambda a, b: own[a, pl.ds(b, 1), :], lambda b: halves(now, b, at)),
                (lambda a, b: cross[a, pl.ds(b, 1), :], lambda b: halves(other, b, at)),
            ],
            store,
            lambda a: [0.85 * x for x in jnp.split(now[at, row16(a), :], 2)],
        )

    section(jnp.int32(0), first.at[0], first.at[1])

    def later(k, carry):
        copy(k).wait()

        @pl.when(k < SECTIONS - 1)
        def _():
            copy(k + 1).start()

        section(k, maps.at[k & 1, 0], maps.at[k & 1, 1])
        return carry

    lax.fori_loop(1, SECTIONS, later, 0)

    square = jnp.zeros((NRHS, 128), F32)
    inner = jnp.zeros((NRHS, 128), F32)
    for t in range(2):
        accs = [None] * 16
        for w in range(WIDTH):
            vec = now[0, pl.ds(w * 16, 16), :]
            for i in range(16):
                s = t * 16 + i
                term = leaf_ref[w, s : s + 1, :] * vec
                accs[i] = term if accs[i] is None else accs[i] + term
        for i in range(16):
            s = t * 16 + i
            v = points_ref[pl.ds(s * 16, 16), :]
            x = points_ref[pl.ds(512 + s * 8 + 2, 1), :] * v + accs[i]
            image[pl.ds(s * 16, 16), :] = x
            square += v * v
            inner += v * x
            sign = 2.0 * points_ref[pl.ds(512 + s * 8 + 4, 1), :] - 1.0
            high = points_ref[pl.ds(512 + s * 8 + 3, 1), :].astype(jnp.int32) >> 8
            split_rows(lhs, x * sign, high, pl.ds(s * 128, 128))
    sums = state_rows([square, inner])
    valid = lane < 16
    vv = jnp.where(valid, sums, 0.0)
    iv = jnp.where(valid, pltpu.roll(sums, 112, 1), 0.0)
    local = jnp.where(vv > 0.0, iv / jnp.where(vv > 0.0, vv, 1.0), 0.0)
    across = jnp.broadcast_to(local, (128, 128)).T[0:NRHS, :]
    energy = jnp.zeros((NRHS, 128), F32)
    mixed = jnp.zeros((NRHS, 128), F32)
    for s in range(LEAF):
        v = points_ref[pl.ds(s * 16, 16), :]
        r = image[pl.ds(s * 16, 16), :] - across * v
        energy += r * r
        mixed += r * v
    for c in range(4):
        image_ref[pl.ds(c * 128, 128), :] = image[pl.ds(c * 128, 128), :].T
    for half, tile in enumerate(sketched(lhs, rhs)):
        out_ref[pl.ds(half, 128, stride=SUM_ROWS), :] = tile
    out_ref[pl.ds(2, 128, stride=SUM_ROWS), :] = keep_ref[...] + taken_ref[...]
    rest = jnp.where(lane < 32, state_rows([energy, mixed]), 0.0)
    state = vv + pltpu.roll(local, 16, 1) + pltpu.roll(rest, 32, 1)
    out_ref[pl.ds(3, 128, stride=SUM_ROWS), :] = jnp.broadcast_to(state, (128, 128))


def merged(vv, p, e, cr, total):
    square = total(vv)
    inner = total(p * vv + cr)
    local = jnp.where(square > 0.0, inner / jnp.where(square > 0.0, square, 1.0), 0.0)
    return square, inner, local


def moved_energy(vv, p, e, cr, at, total):
    off = p - at
    return total(e + off * (2.0 * cr + off * vv)), total(cr + off * vv)


def sum_kernel(info_ref, got_ref, out_ref):
    sums = [
        jnp.sum(got_ref[pl.ds(c, 128, stride=SUM_ROWS), :], axis=0, keepdims=True)
        for c in range(3)
    ]
    first = info_ref[2:3, :] == 0
    out_ref[0:1, :] = sums[0]
    out_ref[1:2, :] = sums[1]
    out_ref[2:3, :] = jnp.where(first, sums[2], 0.0)
    out_ref[3:4, :] = jnp.where(first, 0.0, sums[2])
    state = got_ref[pl.ds(3, 128, stride=SUM_ROWS), :]
    valid = lax.broadcasted_iota(jnp.int32, (128, 128), 1) < 16
    parts = [
        jnp.where(valid, pltpu.roll(state, (128 - 16 * i) % 128, 1) if i else state, 0.0)
        for i in range(4)
    ]

    def total(x):
        return jnp.sum(x, axis=0, keepdims=True)

    square, inner, local = merged(*parts, total)
    energy, mixed = moved_energy(*parts, local, total)
    for i, x in enumerate((square, local, energy, mixed)):
        out_ref[4 + i : 5 + i, :] = x


def chunk_kernel(mine_ref, theirs_ref, image_ref, out_ref, arnoldi_ref, scalars_ref):
    for c in range(4):
        out_ref[pl.ds(c, 128, stride=BACK_ROWS), :] = image_ref[pl.ds(c * 128, 128), :]
    both = [(mine_ref[4 + i : 5 + i, :], theirs_ref[4 + i : 5 + i, :]) for i in range(4)]
    vv, p, e, cr = both
    square = vv[0] + vv[1]
    inner = (p[0] * vv[0] + cr[0]) + (p[1] * vv[1] + cr[1])
    proj = (inner / NPTS) / (square / NPTS + EPS)
    terms = []
    for i in range(2):
        off = p[i] - proj
        terms.append(e[i] + off * (2.0 * cr[i] + off * vv[i]))
    spread = jnp.sqrt(jnp.maximum(terms[0] + terms[1], 0.0) / NPTS + EPS)
    arnoldi_ref[0:1, :] = proj[:, 0:NRHS]
    arnoldi_ref[1:2, :] = spread[:, 0:NRHS]
    valid = lax.broadcasted_iota(jnp.int32, (1, 128), 1) < 16

    def tiled(x):
        x = jnp.where(valid, x, 0.0)
        for shift in (16, 32, 64):
            x = x + pltpu.roll(x, shift, 1)
        return x

    proj, spread = tiled(proj), tiled(spread)
    scalars_ref[0:1, :] = proj
    scalars_ref[1:2, :] = spread
    sums = mine_ref[0:4, :] + theirs_ref[0:4, :]
    chunk = (sums[0:2] - proj * sums[2:4]) / spread * math.sqrt(SKETCH / NPTS)
    for i in range(2):
        out_ref[pl.ds(4 + i, 128, stride=BACK_ROWS), :] = jnp.broadcast_to(
            chunk[i : i + 1], (128, 128)
        )


def last_kernel(got_ref, scalars_ref, v_ref, basis_ref, sketch_ref, turned):
    proj = jnp.broadcast_to(scalars_ref[0:1, :], (128, 128)).T[0:NRHS, :]
    spread = jnp.broadcast_to(scalars_ref[1:2, :], (128, 128)).T[0:NRHS, :]
    lane = lax.broadcasted_iota(jnp.int32, (32, 128), 1) & -16
    for c in range(4):
        blocks = []
        for jt in range(4):
            rows = got_ref[pl.ds(jt * 32 * BACK_ROWS + c, 32, stride=BACK_ROWS), :]
            blocks.append(pltpu.roll(rows, jt * 32, 1) if jt else rows)
        for m in range(8):
            made = blocks[0]
            for jt in range(1, 4):
                made = jnp.where(lane == (jt * 32 + m * 16) % 128, blocks[jt], made)
            made = pltpu.roll(made, 128 - m * 16, 1) if m else made
            turned[pl.ds(c * 8 + m, 32, stride=32), :] = made
    for jb in range(8):
        back = turned[pl.ds(jb * 128, 128), :].T
        for jt in range(4):
            cols = pl.ds((jb * 4 + jt) * 128, 128)
            x = back[jt * 32 : jt * 32 + 16, :]
            basis_ref[:, cols] = (x - proj * v_ref[:, cols]) / spread
    for half in range(2):
        tile = got_ref[pl.ds(4 + half, 128, stride=BACK_ROWS), :].T
        for t in range(8):
            sketch_ref[:, pl.ds((half * 8 + t) * 128, 128)] = tile[t * 16 : t * 16 + 16, :]


VMEM = pl.BlockSpec(memory_space=pltpu.VMEM)
HBM = pl.BlockSpec(memory_space=pltpu.HBM)


def f32(*shape):
    return jax.ShapeDtypeStruct(shape, F32)


def call(kernel, out, ins, scratch=(), flops=1000000, mib=12, outs=None):
    single = not isinstance(out, tuple)
    return pl.pallas_call(
        kernel,
        out_shape=out,
        in_specs=ins,
        out_specs=outs or (VMEM if single else tuple(VMEM for _ in out)),
        scratch_shapes=list(scratch),
        cost_estimate=pl.CostEstimate(flops=flops, bytes_accessed=1000000, transcendentals=0),
        compiler_params=pltpu.CompilerParams(vmem_limit_bytes=mib * 1024 * 1024),
    )


def exchange(x):
    return lax.all_to_all(x[:, None, :], CHIP, 0, 0, tiled=True)[:, 0, :]


def body(basis_vector, diagonal, coords, phase_scale, sketch_rows, sketch_signs):
    chip = lax.axis_index(CHIP)
    core = lax.axis_index(CORE)
    info = jnp.stack([phase_scale[0] % MOD, chip, core] + [core] * 5).astype(jnp.int32)
    info = jnp.broadcast_to(info[:, None], (8, 128))
    points = LEAF * CHIPS
    swap = [(0, 1), (1, 0)]
    sketch_rows, sketch_signs = sketch_rows.reshape(32, 128), sketch_signs.reshape(32, 128)
    vector = pltpu.VMEM((NRHS, points), F32)
    ints = pltpu.VMEM((32, 128), jnp.int32)
    turned = pltpu.VMEM((1024, 128), F32)
    parts = pltpu.VMEM((256, points), jnp.bfloat16)
    hot_type = jax.ShapeDtypeStruct((256, points), jnp.bfloat16)
    packed = call(
        pack_kernel,
        f32(CHIPS * OUT_ROWS, 128),
        [HBM] * 5,
        [
            vector,
            pltpu.VMEM((2, points), jnp.int32),
            pltpu.VMEM((32, 128), F32),
            ints,
            ints,
            turned,
            pltpu.SemaphoreType.DMA((5,)),
        ],
        mib=60,
    )(basis_vector, coords, diagonal.reshape(32, 128), sketch_rows, sketch_signs)
    map_pair = pltpu.VMEM((2, 2, WIDTH, WIDTH, 128), F32)
    tile = f32(CHIPS, 128)
    maps, keep, give = call(
        early_kernel,
        (f32(SECTIONS - 1, 2, WIDTH, WIDTH, 128), tile, tile),
        [VMEM] + [HBM] * 3,
        [
            vector,
            ints,
            ints,
            map_pair,
            parts,
            parts,
            pltpu.SemaphoreType.DMA((3,)),
            pltpu.SemaphoreType.DMA((2,)),
        ],
        outs=(HBM, VMEM, VMEM),
        flops=20000000,
        mib=EARLY_MIB,
    )(info, basis_vector, sketch_rows, sketch_signs)
    got = exchange(packed)
    taken = lax.ppermute(give, CORE, swap)
    coeffs, leaf, held = call(
        leaf_kernel,
        (f32(512, 128), f32(WIDTH, LEAF, 128), f32(OUT_ROWS * 128, 128)),
        [VMEM, VMEM, HBM],
    )(info, got, keep)
    partner = lax.ppermute(coeffs, CORE, swap)
    first_type = f32(2, WIDTH, WIDTH, 128)
    hot, first = call(hot_kernel, (hot_type, first_type), [VMEM, VMEM])(info, held)
    pair = pltpu.VMEM((2, 512, 128), F32)
    parts_out, image = call(
        core_kernel,
        (f32(CHIPS * SUM_ROWS, 128), f32(512, 128)),
        [VMEM] * 8 + [HBM],
        [
            pair,
            pair,
            pltpu.VMEM((512, 128), F32),
            parts,
            map_pair,
            pltpu.SemaphoreType.DMA((2,)),
        ],
        mib=CORE_MIB,
    )(coeffs, partner, leaf, held, first, hot, keep, taken, maps)
    mine = call(sum_kernel, f32(8, 128), [VMEM, VMEM])(info, exchange(parts_out))
    theirs = lax.ppermute(mine, CORE, swap)
    back, arnoldi, scalars = call(
        chunk_kernel, (f32(CHIPS * BACK_ROWS, 128), f32(2, NRHS), f32(2, 128)), [VMEM] * 3
    )(mine, theirs, image)
    new_basis, sketch = call(
        last_kernel, (f32(NRHS, points), f32(NRHS, SKETCH)), [VMEM] * 3, [turned]
    )(exchange(back), scalars, basis_vector)
    return new_basis, sketch, arnoldi


def solution(mesh):
    torus = Mesh(mesh.devices.reshape(4, 8, 4, 2), ("box_0", "box_1", "box_2", "box_3"))
    box = ("box_0", "box_1", "box_2", "box_3")
    placed = (P(None, box), P(box), P(None, box), P(), P(box), P(box))
    return jax.shard_map(
        body, mesh=torus, in_specs=placed, out_specs=(P(None, box), P(), P()), check_vma=False
    )
```

```python
import functools
import math

import jax
import jax.numpy as jnp
from jax import lax
from jax.experimental import pallas as pl
from jax.experimental.pallas import tpu as pltpu
from jax.sharding import Mesh
from jax.sharding import PartitionSpec as P

RANK = 16
WIDTH = 32
LEAF = 32
SKETCH = 2048
NRHS = 16
SECTIONS = 8
CHIPS = 128
NPTS = 1048576
MOD = 8191
EPS = 1e-06
CHIP = ("box_0", "box_1", "box_2")
CORE = "box_3"
OUT_ROWS = 6
SUM_ROWS = 4
BACK_ROWS = 6
EARLY_MIB = 48
CORE_MIB = 47
F32 = jnp.float32


def fold(x):
    return (x & MOD) + (x >> 13)


def unit_circle(phase):
    r = phase.astype(F32)
    r = jnp.where(r > 4095.5, r - float(MOD), r)
    y = r * (math.pi / MOD)
    y2 = y * y
    s = 1.0 / math.factorial(13)
    for k in (11, 9, 7, 5, 3, 1):
        s = s * y2 + (-1.0) ** (k // 2) / math.factorial(k)
    s = s * y
    c = -1.0 / math.factorial(14)
    for k in (12, 10, 8, 6, 4, 2, 0):
        c = c * y2 + (-1.0) ** (k // 2) / math.factorial(k)
    return 1.0 - 2.0 * s * s, 2.0 * s * c


def times(a, b):
    return a[0] * b[0] - a[1] * b[1], a[0] * b[1] + a[1] * b[0]


def split_rows(lhs, y, high, cols):
    top = y.astype(jnp.bfloat16).astype(F32)
    for p, part in enumerate((top, y - top)):
        for h in range(8):
            mask = jnp.broadcast_to(high == h, (NRHS, 128))
            lhs[pl.ds(p * 128 + h * 16, 16), cols] = jnp.where(mask, part, 0.0).astype(jnp.bfloat16)


def hot_rows(rhs, low, cols):
    index = lax.broadcasted_iota(jnp.int32, (256, 128), 0)
    rhs[:, cols] = jnp.where(index == low, 1.0, 0.0).astype(jnp.bfloat16)


def sketched(lhs, rhs):
    both = lax.dot_general(
        lhs[...], rhs[...], (((1,), (1,)), ((), ())), preferred_element_type=F32
    )
    both = both[0:128] + both[128:256]
    return [
        jnp.concatenate(
            [
                both[(t // 2) * 16 : (t // 2) * 16 + 16, (t % 2) * 128 : (t % 2) * 128 + 128]
                for t in range(half * 8, half * 8 + 8)
            ],
            0,
        ).T
        for half in range(2)
    ]


def fetches(sources, held, sems):
    return [pltpu.make_async_copy(a, b, sems.at[i]) for i, (a, b) in enumerate(zip(sources, held))]


def pack_kernel(*refs):
    sources, out_ref, held, turned, sems = refs[:5], refs[5], refs[6:11], refs[11], refs[12]
    copies = fetches(sources, held, sems)
    for copy in copies:
        copy.start()
    for copy in copies:
        copy.wait()
    v_ref, coords_ref, diag_ref, rows_ref, signs_ref = held
    zeros = jnp.zeros((11, 128), F32)
    for jb in range(8):
        tiles = []
        for jt in range(4):
            j = jb * 4 + jt
            cols = pl.ds(j * 128, 128)
            tiles += [
                v_ref[:, cols],
                coords_ref[:, cols].astype(F32),
                diag_ref[j : j + 1, :],
                rows_ref[j : j + 1, :].astype(F32),
                signs_ref[j : j + 1, :].astype(F32),
                zeros,
            ]
        turned[pl.ds(jb * 128, 128), :] = jnp.concatenate(tiles, 0).T
    lane = lax.broadcasted_iota(jnp.int32, (32, 128), 1)
    made = {}
    for s in range(LEAF):
        rows = turned[pl.ds(s, 32, stride=32), :]
        for col, start, width, at in (
            (s // 8, 0, 16, 16 * (s % 8)),
            (4 + s // 16, 16, 8, 8 * (s % 16)),
        ):
            moved = pltpu.roll(rows, at, 1) if at else rows
            for jt in range(4):
                first = (jt * 32 + start + at) % 128
                if (col, jt) in made:
                    moved_here = jnp.where((lane & -width) == first, moved, made[col, jt])
                else:
                    moved_here = moved
                made[col, jt] = moved_here
    for (col, jt), rows in made.items():
        shift = (-jt * 32 - (16 if col >= 4 else 0)) % 128
        rows = pltpu.roll(rows, shift, 1) if shift else rows
        out_ref[pl.ds(jt * 32 * OUT_ROWS + col, 32, stride=OUT_ROWS), :] = rows


def product(out_count, terms, store, start=None, width=16, group=16):
    def tile(t, carry):
        accs = [jnp.zeros((8, 128), F32)] * (2 * width)
        if start is not None:
            accs = [x for i in range(width) for x in start(t * width + i)]

        def some(g, accs):
            accs = list(accs)
            for matrix, vector in terms:
                for i in range(group):
                    b = g * group + i
                    vec = vector(b)
                    for i in range(width):
                        row = jnp.broadcast_to(matrix(t * width + i, b), (8, 128))
                        for half in range(2):
                            accs[2 * i + half] += row * vec[half]
            return tuple(accs)

        accs = lax.fori_loop(0, 32 // group, some, tuple(accs))
        for i in range(width):
            store(t * width + i, accs[2 * i : 2 * i + 2])
        return carry

    lax.fori_loop(0, out_count // width, tile, 0)


def halves(ref, a, *lead):
    return [ref[(*lead, pl.ds(pl.multiple_of(a * 16 + 8 * h, 8), 8), slice(None))] for h in range(2)]


def row16(a):
    return pl.ds(pl.multiple_of(a * 16, 16), 16)


def leaf_kernel(info_ref, got_ref, after_ref, coeffs_ref, leaf_ref, points_ref):
    for c in range(6):
        points_ref[pl.ds(c * 128, 128), :] = got_ref[pl.ds(c, 128, stride=OUT_ROWS), :].T
    scale = info_ref[0:1, :]

    def powers(field):
        where = points_ref[pl.ds(512 + field, 32, stride=8), :].astype(jnp.int32)
        one = unit_circle(fold(fold(where * scale)))
        two = times(one, one)
        return [one, two, times(two, one), times(two, two)]

    first, second = powers(0), powers(1)
    gain = 1.0 / math.sqrt(LEAF)
    second = [(c * gain, s * gain) for c, s in second]
    for w in range(RANK):
        c, s = times(first[w % 4], second[w // 4])
        leaf_ref[w] = c
        leaf_ref[w + RANK] = s

    def store(a, x):
        coeffs_ref[row16(a), :] = jnp.concatenate(x, 0)

    product(
        WIDTH,
        [(lambda a, b: leaf_ref[a, pl.ds(b, 1), :], lambda b: halves(points_ref, b))],
        store,
    )


def section_map(map_ref, unit, offset, first_power, turn, gain):
    index = lax.broadcasted_iota(jnp.int32, (WIDTH, 128), 0) + offset
    one = unit_circle(fold(fold(unit * index)))
    two = times(one, one)
    four = times(two, two)
    scale = (gain * math.cos(turn), gain * math.sin(turn))
    power = one if first_power == 1 else times(two, one)
    power = (
        power[0] * scale[0] - power[1] * scale[1],
        power[0] * scale[1] + power[1] * scale[0],
    )
    fine = [power]
    for _ in range(3):
        fine.append(times(fine[-1], one))
    coarse = None
    for i in range(8):
        for j in range(4):
            c, s = fine[j]
            map_ref[4 * i + j] = c if coarse is None else coarse[0] * c - coarse[1] * s
        coarse = four if coarse is None else times(coarse, four)


def state_rows(parts):
    pad = [jnp.zeros((128 - 16 * len(parts), 128), F32)]
    return jnp.sum(jnp.concatenate(parts + pad, 0).T, axis=0, keepdims=True)


def section_maps(info_ref, k, maps_ref):
    scale, chip, core = info_ref[0:1, :], info_ref[1:2, :], info_ref[2:3, :]
    place = ((chip >> 2) & 7) * 16 + (chip >> 5) * 4 + (chip & 3)
    lane = lax.broadcasted_iota(jnp.int32, (1, 128), 1)
    key = ((lane * 2 + core) * 128 + place) * 37 + 101 * k
    whole = (key.astype(F32) * (1.0 / (MOD - 1))).astype(jnp.int32)
    key = key - whole * (MOD - 1)
    key = jnp.where(key < 0, key + (MOD - 1), key)
    key = jnp.where(key >= MOD - 1, key - (MOD - 1), key)
    unit = fold(fold((key + 1) * scale))
    turn = 2.0 * math.pi * 4096 / MOD
    section_map(maps_ref.at[0], unit, 2, 1, 0.0, 0.35 / math.sqrt(WIDTH))
    section_map(maps_ref.at[1], unit, 1, 3, turn, 0.6 / math.sqrt(WIDTH))


def early_kernel(info_ref, *refs):
    sources, maps_hbm, keep_ref, give_ref = refs[:3], *refs[3:6]
    held, maps, lhs, rhs, sems, map_sems = refs[6:9], *refs[9:]
    copies = fetches(sources, held, sems)
    for copy in copies:
        copy.start()

    def leave(k):
        return pltpu.make_async_copy(maps.at[k & 1], maps_hbm.at[k - 1], map_sems.at[k & 1])

    def section(k, carry):
        @pl.when(k > 2)
        def _():
            leave(k - 2).wait()

        section_maps(info_ref, k, maps.at[k & 1])
        leave(k).start()
        return carry

    lax.fori_loop(1, SECTIONS, section, 0)
    for copy in copies:
        copy.wait()
    v_ref, rows_ref, signs_ref = held
    for j in range(32):
        cols = pl.ds(j * 128, 128)
        rows, signs = rows_ref[j : j + 1, :], signs_ref[j : j + 1, :]
        split_rows(lhs, v_ref[:, cols] * (2 * signs - 1).astype(F32), rows >> 8, cols)
        hot_rows(rhs, rows & 255, cols)
    low, high = sketched(lhs, rhs)
    first = info_ref[2:3, :] == 0
    first = jnp.broadcast_to(first, (128, 128))
    keep_ref[...] = jnp.where(first, low, high)
    give_ref[...] = jnp.where(first, high, low)
    for k in (SECTIONS - 2, SECTIONS - 1):
        leave(k).wait()


def hot_kernel(info_ref, points_ref, rhs_ref, maps_ref):
    for s in range(LEAF):
        low = points_ref[pl.ds(512 + s * 8 + 3, 1), :].astype(jnp.int32) & 255
        hot_rows(rhs_ref, low, pl.ds(s * 128, 128))
    section_maps(info_ref, 0, maps_ref)


def core_kernel(
    coeffs_ref,
    partner_ref,
    leaf_ref,
    points_ref,
    first,
    rhs,
    keep_ref,
    taken_ref,
    maps_hbm,
    out_ref,
    image_ref,
    now,
    other,
    image,
    lhs,
    maps,
    sems,
):
    lane = lax.broadcasted_iota(jnp.int32, (1, 128), 1)
    lanes = lax.broadcasted_iota(jnp.int32, (8, 128), 1)

    def copy(k):
        slot = lax.rem(k, 3)
        return pltpu.make_async_copy(maps_hbm.at[k - 1], maps.at[slot], sems.at[slot])

    copy(jnp.int32(1)).start()
    copy(jnp.int32(2)).start()
    now[0] = coeffs_ref[...]
    other[0] = partner_ref[...]

    def section(k, own, cross):
        at = k & 1
        step = jnp.left_shift(1, jnp.minimum(k, SECTIONS - 2))
        across = lanes ^ step

        def store(a, x):
            now[1 - at, row16(a), :] = jnp.concatenate(x, 0)
            other[1 - at, row16(a), :] = jnp.concatenate(
                [jnp.take_along_axis(y, across, axis=1, mode="promise_in_bounds") for y in x], 0
            )

        product(
            WIDTH,
            [
                (lambda a, b: own[a, pl.ds(b, 1), :], lambda b: halves(now, b, at)),
                (lambda a, b: cross[a, pl.ds(b, 1), :], lambda b: halves(other, b, at)),
            ],
            store,
            lambda a: [0.85 * x for x in jnp.split(now[at, row16(a), :], 2)],
        )

    section(jnp.int32(0), first.at[0], first.at[1])

    def later(k, carry):
        copy(k).wait()

        @pl.when(k < SECTIONS - 2)
        def _():
            copy(k + 2).start()

        slot = lax.rem(k, 3)
        section(k, maps.at[slot, 0], maps.at[slot, 1])
        return carry

    lax.fori_loop(1, SECTIONS, later, 0)

    def apply(s, x):
        at = pl.multiple_of(512 + s * 8, 8)
        diagonal = points_ref[pl.ds(at, 8), :][2:3, :]
        image[row16(s), :] = diagonal * points_ref[row16(s), :] + jnp.concatenate(x, 0)

    product(
        LEAF,
        [(lambda a, b: leaf_ref[b, pl.ds(a, 1), :], lambda b: halves(now, b, 0))],
        apply,
    )
    square = jnp.zeros((NRHS, 128), F32)
    inner = jnp.zeros((NRHS, 128), F32)
    for s in range(LEAF):
        v = points_ref[pl.ds(s * 16, 16), :]
        x = image[pl.ds(s * 16, 16), :]
        square += v * v
        inner += v * x
        sign = 2.0 * points_ref[pl.ds(512 + s * 8 + 4, 1), :] - 1.0
        high = points_ref[pl.ds(512 + s * 8 + 3, 1), :].astype(jnp.int32) >> 8
        split_rows(lhs, x * sign, high, pl.ds(s * 128, 128))
    sums = state_rows([square, inner])
    valid = lane < 16
    vv = jnp.where(valid, sums, 0.0)
    iv = jnp.where(valid, pltpu.roll(sums, 112, 1), 0.0)
    local = jnp.where(vv > 0.0, iv / jnp.where(vv > 0.0, vv, 1.0), 0.0)
    across = jnp.broadcast_to(local, (128, 128)).T[0:NRHS, :]
    energy = jnp.zeros((NRHS, 128), F32)
    mixed = jnp.zeros((NRHS, 128), F32)
    for s in range(LEAF):
        v = points_ref[pl.ds(s * 16, 16), :]
        r = image[pl.ds(s * 16, 16), :] - across * v
        energy += r * r
        mixed += r * v
    for c in range(4):
        image_ref[pl.ds(c * 128, 128), :] = image[pl.ds(c * 128, 128), :].T
    for half, tile in enumerate(sketched(lhs, rhs)):
        out_ref[pl.ds(half, 128, stride=SUM_ROWS), :] = tile
    out_ref[pl.ds(2, 128, stride=SUM_ROWS), :] = keep_ref[...] + taken_ref[...]
    rest = jnp.where(lane < 32, state_rows([energy, mixed]), 0.0)
    state = vv + pltpu.roll(local, 16, 1) + pltpu.roll(rest, 32, 1)
    out_ref[pl.ds(3, 128, stride=SUM_ROWS), :] = jnp.broadcast_to(state, (128, 128))


def merged(vv, p, e, cr, total):
    square = total(vv)
    inner = total(p * vv + cr)
    local = jnp.where(square > 0.0, inner / jnp.where(square > 0.0, square, 1.0), 0.0)
    return square, inner, local


def moved_energy(vv, p, e, cr, at, total):
    off = p - at
    return total(e + off * (2.0 * cr + off * vv)), total(cr + off * vv)


def sum_kernel(info_ref, got_ref, out_ref):
    sums = [
        jnp.sum(got_ref[pl.ds(c, 128, stride=SUM_ROWS), :], axis=0, keepdims=True)
        for c in range(3)
    ]
    first = info_ref[2:3, :] == 0
    out_ref[0:1, :] = sums[0]
    out_ref[1:2, :] = sums[1]
    out_ref[2:3, :] = jnp.where(first, sums[2], 0.0)
    out_ref[3:4, :] = jnp.where(first, 0.0, sums[2])
    state = got_ref[pl.ds(3, 128, stride=SUM_ROWS), :]
    valid = lax.broadcasted_iota(jnp.int32, (128, 128), 1) < 16
    parts = [
        jnp.where(valid, pltpu.roll(state, (128 - 16 * i) % 128, 1) if i else state, 0.0)
        for i in range(4)
    ]

    def total(x):
        return jnp.sum(x, axis=0, keepdims=True)

    square, inner, local = merged(*parts, total)
    energy, mixed = moved_energy(*parts, local, total)
    for i, x in enumerate((square, local, energy, mixed)):
        out_ref[4 + i : 5 + i, :] = x


def chunk_kernel(mine_ref, theirs_ref, image_ref, out_ref, arnoldi_ref, scalars_ref):
    for c in range(4):
        out_ref[pl.ds(c, 128, stride=BACK_ROWS), :] = image_ref[pl.ds(c * 128, 128), :]
    both = [(mine_ref[4 + i : 5 + i, :], theirs_ref[4 + i : 5 + i, :]) for i in range(4)]
    vv, p, e, cr = both
    square = vv[0] + vv[1]
    inner = (p[0] * vv[0] + cr[0]) + (p[1] * vv[1] + cr[1])
    proj = (inner / NPTS) / (square / NPTS + EPS)
    terms = []
    for i in range(2):
        off = p[i] - proj
        terms.append(e[i] + off * (2.0 * cr[i] + off * vv[i]))
    spread = jnp.sqrt(jnp.maximum(terms[0] + terms[1], 0.0) / NPTS + EPS)
    arnoldi_ref[0:1, :] = proj[:, 0:NRHS]
    arnoldi_ref[1:2, :] = spread[:, 0:NRHS]
    valid = lax.broadcasted_iota(jnp.int32, (1, 128), 1) < 16

    def tiled(x):
        x = jnp.where(valid, x, 0.0)
        for shift in (16, 32, 64):
            x = x + pltpu.roll(x, shift, 1)
        return x

    proj, spread = tiled(proj), tiled(spread)
    scalars_ref[0:1, :] = proj
    scalars_ref[1:2, :] = spread
    sums = mine_ref[0:4, :] + theirs_ref[0:4, :]
    chunk = (sums[0:2] - proj * sums[2:4]) / spread * math.sqrt(SKETCH / NPTS)
    for i in range(2):
        out_ref[pl.ds(4 + i, 128, stride=BACK_ROWS), :] = jnp.broadcast_to(
            chunk[i : i + 1], (128, 128)
        )


def last_kernel(got_ref, scalars_ref, v_ref, basis_hbm, sketch_hbm, turned, basis_ref, sketch_ref, sems):
    for half in range(2):
        tile = got_ref[pl.ds(4 + half, 128, stride=BACK_ROWS), :].T
        for t in range(8):
            sketch_ref[:, pl.ds((half * 8 + t) * 128, 128)] = tile[t * 16 : t * 16 + 16, :]
    copies = [pltpu.make_async_copy(sketch_ref, sketch_hbm, sems.at[8])]
    copies[0].start()
    proj = jnp.broadcast_to(scalars_ref[0:1, :], (128, 128)).T[0:NRHS, :]
    gain = jnp.broadcast_to(1.0 / scalars_ref[1:2, :], (128, 128)).T[0:NRHS, :]
    lane = lax.broadcasted_iota(jnp.int32, (32, 128), 1) & -16
    for c in range(4):
        blocks = []
        for jt in range(4):
            rows = got_ref[pl.ds(jt * 32 * BACK_ROWS + c, 32, stride=BACK_ROWS), :]
            blocks.append(pltpu.roll(rows, jt * 32, 1) if jt else rows)
        for m in range(8):
            made = blocks[0]
            for jt in range(1, 4):
                made = jnp.where(lane == (jt * 32 + m * 16) % 128, blocks[jt], made)
            made = pltpu.roll(made, 128 - m * 16, 1) if m else made
            turned[pl.ds(c * 8 + m, 32, stride=32), :] = made
    for jb in range(8):
        back = turned[pl.ds(jb * 128, 128), :].T
        for jt in range(4):
            cols = pl.ds((jb * 4 + jt) * 128, 128)
            x = back[jt * 32 : jt * 32 + 16, :]
            basis_ref[:, cols] = (x - proj * v_ref[:, cols]) * gain
        cols = pl.ds(jb * 512, 512)
        copies.append(
            pltpu.make_async_copy(basis_ref.at[:, cols], basis_hbm.at[:, cols], sems.at[jb])
        )
        copies[-1].start()
    for copy in copies:
        copy.wait()


VMEM = pl.BlockSpec(memory_space=pltpu.VMEM)
HBM = pl.BlockSpec(memory_space=pltpu.HBM)


def f32(*shape):
    return jax.ShapeDtypeStruct(shape, F32)


def call(kernel, out, ins, scratch=(), flops=1000000, mib=12, outs=None):
    single = not isinstance(out, tuple)
    return pl.pallas_call(
        kernel,
        out_shape=out,
        in_specs=ins,
        out_specs=outs or (VMEM if single else tuple(VMEM for _ in out)),
        scratch_shapes=list(scratch),
        cost_estimate=pl.CostEstimate(flops=flops, bytes_accessed=1000000, transcendentals=0),
        compiler_params=pltpu.CompilerParams(vmem_limit_bytes=mib * 1024 * 1024),
    )


def exchange(x):
    return lax.all_to_all(x[:, None, :], CHIP, 0, 0, tiled=True)[:, 0, :]


def body(basis_vector, diagonal, coords, phase_scale, sketch_rows, sketch_signs):
    chip = lax.axis_index(CHIP)
    core = lax.axis_index(CORE)
    info = jnp.stack([phase_scale[0] % MOD, chip, core] + [core] * 5).astype(jnp.int32)
    info = jnp.broadcast_to(info[:, None], (8, 128))
    points = LEAF * CHIPS
    swap = [(0, 1), (1, 0)]
    sketch_rows, sketch_signs = sketch_rows.reshape(32, 128), sketch_signs.reshape(32, 128)
    vector = pltpu.VMEM((NRHS, points), F32)
    ints = pltpu.VMEM((32, 128), jnp.int32)
    turned = pltpu.VMEM((1024, 128), F32)
    parts = pltpu.VMEM((256, points), jnp.bfloat16)
    hot_type = jax.ShapeDtypeStruct((256, points), jnp.bfloat16)
    packed = call(
        pack_kernel,
        f32(CHIPS * OUT_ROWS, 128),
        [HBM] * 5,
        [
            vector,
            pltpu.VMEM((2, points), jnp.int32),
            pltpu.VMEM((32, 128), F32),
            ints,
            ints,
            turned,
            pltpu.SemaphoreType.DMA((5,)),
        ],
        mib=60,
    )(basis_vector, coords, diagonal.reshape(32, 128), sketch_rows, sketch_signs)
    map_pair = pltpu.VMEM((2, 2, WIDTH, WIDTH, 128), F32)
    tile = f32(CHIPS, 128)
    maps, keep, give = call(
        early_kernel,
        (f32(SECTIONS - 1, 2, WIDTH, WIDTH, 128), tile, tile),
        [VMEM] + [HBM] * 3,
        [
            vector,
            ints,
            ints,
            map_pair,
            parts,
            parts,
            pltpu.SemaphoreType.DMA((3,)),
            pltpu.SemaphoreType.DMA((2,)),
        ],
        outs=(HBM, VMEM, VMEM),
        flops=20000000,
        mib=EARLY_MIB,
    )(info, basis_vector, sketch_rows, sketch_signs)
    got = exchange(packed)
    taken = lax.ppermute(give, CORE, swap)
    coeffs, leaf, held = call(
        leaf_kernel,
        (f32(512, 128), f32(WIDTH, LEAF, 128), f32(OUT_ROWS * 128, 128)),
        [VMEM, VMEM, HBM],
    )(info, got, keep)
    partner = lax.ppermute(coeffs, CORE, swap)
    first_type = f32(2, WIDTH, WIDTH, 128)
    hot, first = call(hot_kernel, (hot_type, first_type), [VMEM, VMEM])(info, held)
    pair = pltpu.VMEM((2, 512, 128), F32)
    parts_out, image = call(
        core_kernel,
        (f32(CHIPS * SUM_ROWS, 128), f32(512, 128)),
        [VMEM] * 8 + [HBM],
        [
            pair,
            pair,
            pltpu.VMEM((512, 128), F32),
            parts,
            pltpu.VMEM((3, 2, WIDTH, WIDTH, 128), F32),
            pltpu.SemaphoreType.DMA((3,)),
        ],
        mib=CORE_MIB,
    )(coeffs, partner, leaf, held, first, hot, keep, taken, maps)
    mine = call(sum_kernel, f32(8, 128), [VMEM, VMEM])(info, exchange(parts_out))
    theirs = lax.ppermute(mine, CORE, swap)
    back, arnoldi, scalars = call(
        chunk_kernel, (f32(CHIPS * BACK_ROWS, 128), f32(2, NRHS), f32(2, 128)), [VMEM] * 3
    )(mine, theirs, image)
    new_basis, sketch = call(
        last_kernel,
        (f32(NRHS, points), f32(NRHS, SKETCH)),
        [VMEM] * 3,
        [turned, vector, pltpu.VMEM((NRHS, SKETCH), F32), pltpu.SemaphoreType.DMA((9,))],
        outs=(HBM, HBM),
    )(exchange(back), scalars, basis_vector)
    return new_basis, sketch, arnoldi


def solution(mesh):
    torus = Mesh(mesh.devices.reshape(4, 8, 4, 2), ("box_0", "box_1", "box_2", "box_3"))
    box = ("box_0", "box_1", "box_2", "box_3")
    placed = (P(None, box), P(box), P(None, box), P(), P(box), P(box))
    return jax.shard_map(
        body, mesh=torus, in_specs=placed, out_specs=(P(None, box), P(), P()), check_vma=False
    )
```

```python
import functools
import math

import jax
import jax.numpy as jnp
from jax import lax
from jax.experimental import pallas as pl
from jax.experimental.pallas import tpu as pltpu
from jax.sharding import Mesh
from jax.sharding import PartitionSpec as P

RANK = 16
WIDTH = 32
LEAF = 32
SKETCH = 2048
NRHS = 16
SECTIONS = 8
CHIPS = 128
NPTS = 1048576
MOD = 8191
EPS = 1e-06
CHIP = ("box_0", "box_1", "box_2")
CORE = "box_3"
OUT_ROWS = 6
SUM_ROWS = 4
BACK_ROWS = 6
EARLY_MIB = 48
CORE_MIB = 47
F32 = jnp.float32


def fold(x):
    return (x & MOD) + (x >> 13)


def unit_circle(phase):
    r = phase.astype(F32)
    r = jnp.where(r > 4095.5, r - float(MOD), r)
    y = r * (math.pi / MOD)
    y2 = y * y
    s = 1.0 / math.factorial(13)
    for k in (11, 9, 7, 5, 3, 1):
        s = s * y2 + (-1.0) ** (k // 2) / math.factorial(k)
    s = s * y
    c = -1.0 / math.factorial(14)
    for k in (12, 10, 8, 6, 4, 2, 0):
        c = c * y2 + (-1.0) ** (k // 2) / math.factorial(k)
    return 1.0 - 2.0 * s * s, 2.0 * s * c


def times(a, b):
    return a[0] * b[0] - a[1] * b[1], a[0] * b[1] + a[1] * b[0]


def split_rows(lhs, y, high, cols):
    top = y.astype(jnp.bfloat16).astype(F32)
    for p, part in enumerate((top, y - top)):
        for h in range(8):
            mask = jnp.broadcast_to(high == h, (NRHS, 128))
            lhs[pl.ds(p * 128 + h * 16, 16), cols] = jnp.where(mask, part, 0.0).astype(jnp.bfloat16)


def hot_rows(rhs, low, cols):
    index = lax.broadcasted_iota(jnp.int32, (256, 128), 0)
    rhs[:, cols] = jnp.where(index == low, 1.0, 0.0).astype(jnp.bfloat16)


def sketched(lhs, rhs):
    both = lax.dot_general(
        lhs[...], rhs[...], (((1,), (1,)), ((), ())), preferred_element_type=F32
    )
    both = both[0:128] + both[128:256]
    return [
        jnp.concatenate(
            [
                both[(t // 2) * 16 : (t // 2) * 16 + 16, (t % 2) * 128 : (t % 2) * 128 + 128]
                for t in range(half * 8, half * 8 + 8)
            ],
            0,
        ).T
        for half in range(2)
    ]


def fetches(sources, held, sems):
    return [pltpu.make_async_copy(a, b, sems.at[i]) for i, (a, b) in enumerate(zip(sources, held))]


def pack_kernel(*refs):
    sources, out_ref, held, turned, sems = refs[:5], refs[5], refs[6:11], refs[11], refs[12]
    copies = fetches(sources, held, sems)
    for copy in copies:
        copy.start()
    for copy in copies:
        copy.wait()
    v_ref, coords_ref, diag_ref, rows_ref, signs_ref = held
    zeros = jnp.zeros((11, 128), F32)
    for jb in range(8):
        tiles = []
        for jt in range(4):
            j = jb * 4 + jt
            cols = pl.ds(j * 128, 128)
            tiles += [
                v_ref[:, cols],
                coords_ref[:, cols].astype(F32),
                diag_ref[j : j + 1, :],
                rows_ref[j : j + 1, :].astype(F32),
                signs_ref[j : j + 1, :].astype(F32),
                zeros,
            ]
        turned[pl.ds(jb * 128, 128), :] = jnp.concatenate(tiles, 0).T
    lane = lax.broadcasted_iota(jnp.int32, (32, 128), 1)
    made = {}
    for s in range(LEAF):
        rows = turned[pl.ds(s, 32, stride=32), :]
        for col, start, width, at in (
            (s // 8, 0, 16, 16 * (s % 8)),
            (4 + s // 16, 16, 8, 8 * (s % 16)),
        ):
            moved = pltpu.roll(rows, at, 1) if at else rows
            for jt in range(4):
                first = (jt * 32 + start + at) % 128
                if (col, jt) in made:
                    moved_here = jnp.where((lane & -width) == first, moved, made[col, jt])
                else:
                    moved_here = moved
                made[col, jt] = moved_here
    for (col, jt), rows in made.items():
        shift = (-jt * 32 - (16 if col >= 4 else 0)) % 128
        rows = pltpu.roll(rows, shift, 1) if shift else rows
        out_ref[pl.ds(jt * 32 * OUT_ROWS + col, 32, stride=OUT_ROWS), :] = rows


def product(out_count, terms, store, start=None, width=16, group=16):
    def tile(t, carry):
        accs = [jnp.zeros((8, 128), F32)] * (2 * width)
        if start is not None:
            accs = [x for i in range(width) for x in start(t * width + i)]

        def some(g, accs):
            accs = list(accs)
            for matrix, vector in terms:
                for i in range(group):
                    b = g * group + i
                    vec = vector(b)
                    for i in range(width):
                        row = jnp.broadcast_to(matrix(t * width + i, b), (8, 128))
                        for half in range(2):
                            accs[2 * i + half] += row * vec[half]
            return tuple(accs)

        accs = lax.fori_loop(0, 32 // group, some, tuple(accs))
        for i in range(width):
            store(t * width + i, accs[2 * i : 2 * i + 2])
        return carry

    lax.fori_loop(0, out_count // width, tile, 0)


def halves(ref, a, *lead):
    return [ref[(*lead, pl.ds(pl.multiple_of(a * 16 + 8 * h, 8), 8), slice(None))] for h in range(2)]


def row16(a):
    return pl.ds(pl.multiple_of(a * 16, 16), 16)


def leaf_kernel(info_ref, got_ref, after_ref, coeffs_ref, leaf_ref, points_ref):
    for c in range(6):
        points_ref[pl.ds(c * 128, 128), :] = got_ref[pl.ds(c, 128, stride=OUT_ROWS), :].T
    scale = info_ref[0:1, :]

    def powers(field):
        where = points_ref[pl.ds(512 + field, 32, stride=8), :].astype(jnp.int32)
        one = unit_circle(fold(fold(where * scale)))
        two = times(one, one)
        return [one, two, times(two, one), times(two, two)]

    first, second = powers(0), powers(1)
    gain = 1.0 / math.sqrt(LEAF)
    second = [(c * gain, s * gain) for c, s in second]
    for w in range(RANK):
        c, s = times(first[w % 4], second[w // 4])
        leaf_ref[w] = c
        leaf_ref[w + RANK] = s

    def store(a, x):
        coeffs_ref[row16(a), :] = jnp.concatenate(x, 0)

    product(
        WIDTH,
        [(lambda a, b: leaf_ref[a, pl.ds(b, 1), :], lambda b: halves(points_ref, b))],
        store,
    )


def section_map(map_ref, unit, offset, first_power, turn, gain):
    index = lax.broadcasted_iota(jnp.int32, (WIDTH, 128), 0) + offset
    one = unit_circle(fold(fold(unit * index)))
    two = times(one, one)
    four = times(two, two)
    scale = (gain * math.cos(turn), gain * math.sin(turn))
    power = one if first_power == 1 else times(two, one)
    power = (
        power[0] * scale[0] - power[1] * scale[1],
        power[0] * scale[1] + power[1] * scale[0],
    )
    fine = [power]
    for _ in range(3):
        fine.append(times(fine[-1], one))
    coarse = None
    for i in range(8):
        for j in range(4):
            c, s = fine[j]
            map_ref[4 * i + j] = c if coarse is None else coarse[0] * c - coarse[1] * s
        coarse = four if coarse is None else times(coarse, four)


def state_rows(parts):
    pad = [jnp.zeros((128 - 16 * len(parts), 128), F32)]
    return jnp.sum(jnp.concatenate(parts + pad, 0).T, axis=0, keepdims=True)


def section_maps(info_ref, k, maps_ref):
    scale, chip, core = info_ref[0:1, :], info_ref[1:2, :], info_ref[2:3, :]
    place = ((chip >> 2) & 7) * 16 + (chip >> 5) * 4 + (chip & 3)
    lane = lax.broadcasted_iota(jnp.int32, (1, 128), 1)
    key = ((lane * 2 + core) * 128 + place) * 37 + 101 * k
    whole = (key.astype(F32) * (1.0 / (MOD - 1))).astype(jnp.int32)
    key = key - whole * (MOD - 1)
    key = jnp.where(key < 0, key + (MOD - 1), key)
    key = jnp.where(key >= MOD - 1, key - (MOD - 1), key)
    unit = fold(fold((key + 1) * scale))
    turn = 2.0 * math.pi * 4096 / MOD
    section_map(maps_ref.at[0], unit, 2, 1, 0.0, 0.35 / math.sqrt(WIDTH))
    section_map(maps_ref.at[1], unit, 1, 3, turn, 0.6 / math.sqrt(WIDTH))


def early_kernel(info_ref, *refs):
    sources, maps_hbm, keep_ref, give_ref = refs[:3], *refs[3:6]
    held, maps, lhs, rhs, sems, map_sems = refs[6:9], *refs[9:]
    copies = fetches(sources, held, sems)
    for copy in copies:
        copy.start()

    def leave(k):
        return pltpu.make_async_copy(maps.at[k - 1], maps_hbm.at[k - 1], map_sems.at[k - 1])

    def section(k, carry):
        section_maps(info_ref, k, maps.at[k - 1])
        leave(k).start()
        return carry

    lax.fori_loop(1, SECTIONS, section, 0)
    for copy in copies:
        copy.wait()
    v_ref, rows_ref, signs_ref = held
    for j in range(32):
        cols = pl.ds(j * 128, 128)
        rows, signs = rows_ref[j : j + 1, :], signs_ref[j : j + 1, :]
        split_rows(lhs, v_ref[:, cols] * (2 * signs - 1).astype(F32), rows >> 8, cols)
        hot_rows(rhs, rows & 255, cols)
    low, high = sketched(lhs, rhs)
    first = info_ref[2:3, :] == 0
    first = jnp.broadcast_to(first, (128, 128))
    keep_ref[...] = jnp.where(first, low, high)
    give_ref[...] = jnp.where(first, high, low)
    for k in range(1, SECTIONS):
        leave(k).wait()


def hot_kernel(info_ref, points_ref, rhs_ref, maps_ref):
    for s in range(LEAF):
        low = points_ref[pl.ds(512 + s * 8 + 3, 1), :].astype(jnp.int32) & 255
        hot_rows(rhs_ref, low, pl.ds(s * 128, 128))
    section_maps(info_ref, 0, maps_ref)


def core_kernel(
    coeffs_ref,
    partner_ref,
    leaf_ref,
    points_ref,
    first,
    rhs,
    keep_ref,
    taken_ref,
    maps_hbm,
    out_ref,
    image_ref,
    now,
    other,
    image,
    lhs,
    maps,
    sems,
):
    lane = lax.broadcasted_iota(jnp.int32, (1, 128), 1)
    lanes = lax.broadcasted_iota(jnp.int32, (8, 128), 1)

    def copy(k):
        slot = lax.rem(k, 3)
        return pltpu.make_async_copy(maps_hbm.at[k - 1], maps.at[slot], sems.at[slot])

    copy(jnp.int32(1)).start()
    copy(jnp.int32(2)).start()
    now[0] = coeffs_ref[...]
    other[0] = partner_ref[...]

    def section(k, own, cross):
        at = k & 1
        step = jnp.left_shift(1, jnp.minimum(k, SECTIONS - 2))
        across = lanes ^ step

        def store(a, x):
            now[1 - at, row16(a), :] = jnp.concatenate(x, 0)
            other[1 - at, row16(a), :] = jnp.concatenate(
                [jnp.take_along_axis(y, across, axis=1, mode="promise_in_bounds") for y in x], 0
            )

        product(
            WIDTH,
            [
                (lambda a, b: own[a, pl.ds(b, 1), :], lambda b: halves(now, b, at)),
                (lambda a, b: cross[a, pl.ds(b, 1), :], lambda b: halves(other, b, at)),
            ],
            store,
            lambda a: [0.85 * x for x in jnp.split(now[at, row16(a), :], 2)],
        )

    section(jnp.int32(0), first.at[0], first.at[1])

    def later(k, carry):
        copy(k).wait()

        @pl.when(k < SECTIONS - 2)
        def _():
            copy(k + 2).start()

        slot = lax.rem(k, 3)
        section(k, maps.at[slot, 0], maps.at[slot, 1])
        return carry

    lax.fori_loop(1, SECTIONS, later, 0)

    def apply(s, x):
        at = pl.multiple_of(512 + s * 8, 8)
        diagonal = points_ref[pl.ds(at, 8), :][2:3, :]
        image[row16(s), :] = diagonal * points_ref[row16(s), :] + jnp.concatenate(x, 0)

    product(
        LEAF,
        [(lambda a, b: leaf_ref[b, pl.ds(a, 1), :], lambda b: halves(now, b, 0))],
        apply,
    )
    square = jnp.zeros((NRHS, 128), F32)
    inner = jnp.zeros((NRHS, 128), F32)
    for s in range(LEAF):
        v = points_ref[pl.ds(s * 16, 16), :]
        x = image[pl.ds(s * 16, 16), :]
        square += v * v
        inner += v * x
        sign = 2.0 * points_ref[pl.ds(512 + s * 8 + 4, 1), :] - 1.0
        high = points_ref[pl.ds(512 + s * 8 + 3, 1), :].astype(jnp.int32) >> 8
        split_rows(lhs, x * sign, high, pl.ds(s * 128, 128))
    sums = state_rows([square, inner])
    valid = lane < 16
    vv = jnp.where(valid, sums, 0.0)
    iv = jnp.where(valid, pltpu.roll(sums, 112, 1), 0.0)
    local = jnp.where(vv > 0.0, iv / jnp.where(vv > 0.0, vv, 1.0), 0.0)
    across = jnp.broadcast_to(local, (128, 128)).T[0:NRHS, :]
    energy = jnp.zeros((NRHS, 128), F32)
    mixed = jnp.zeros((NRHS, 128), F32)
    for s in range(LEAF):
        v = points_ref[pl.ds(s * 16, 16), :]
        r = image[pl.ds(s * 16, 16), :] - across * v
        energy += r * r
        mixed += r * v
    for c in range(4):
        image_ref[pl.ds(c * 128, 128), :] = image[pl.ds(c * 128, 128), :].T
    for half, tile in enumerate(sketched(lhs, rhs)):
        out_ref[pl.ds(half, 128, stride=SUM_ROWS), :] = tile
    out_ref[pl.ds(2, 128, stride=SUM_ROWS), :] = keep_ref[...] + taken_ref[...]
    rest = jnp.where(lane < 32, state_rows([energy, mixed]), 0.0)
    state = vv + pltpu.roll(local, 16, 1) + pltpu.roll(rest, 32, 1)
    out_ref[pl.ds(3, 128, stride=SUM_ROWS), :] = jnp.broadcast_to(state, (128, 128))


def merged(vv, p, e, cr, total):
    square = total(vv)
    inner = total(p * vv + cr)
    local = jnp.where(square > 0.0, inner / jnp.where(square > 0.0, square, 1.0), 0.0)
    return square, inner, local


def moved_energy(vv, p, e, cr, at, total):
    off = p - at
    return total(e + off * (2.0 * cr + off * vv)), total(cr + off * vv)


def sum_kernel(info_ref, got_ref, out_ref):
    sums = [
        jnp.sum(got_ref[pl.ds(c, 128, stride=SUM_ROWS), :], axis=0, keepdims=True)
        for c in range(3)
    ]
    first = info_ref[2:3, :] == 0
    out_ref[0:1, :] = sums[0]
    out_ref[1:2, :] = sums[1]
    out_ref[2:3, :] = jnp.where(first, sums[2], 0.0)
    out_ref[3:4, :] = jnp.where(first, 0.0, sums[2])
    state = got_ref[pl.ds(3, 128, stride=SUM_ROWS), :]
    valid = lax.broadcasted_iota(jnp.int32, (128, 128), 1) < 16
    parts = [
        jnp.where(valid, pltpu.roll(state, (128 - 16 * i) % 128, 1) if i else state, 0.0)
        for i in range(4)
    ]

    def total(x):
        return jnp.sum(x, axis=0, keepdims=True)

    square, inner, local = merged(*parts, total)
    energy, mixed = moved_energy(*parts, local, total)
    for i, x in enumerate((square, local, energy, mixed)):
        out_ref[4 + i : 5 + i, :] = x


def chunk_kernel(mine_ref, theirs_ref, image_ref, out_ref, arnoldi_ref, scalars_ref):
    for c in range(4):
        out_ref[pl.ds(c, 128, stride=BACK_ROWS), :] = image_ref[pl.ds(c * 128, 128), :]
    both = [(mine_ref[4 + i : 5 + i, :], theirs_ref[4 + i : 5 + i, :]) for i in range(4)]
    vv, p, e, cr = both
    square = vv[0] + vv[1]
    inner = (p[0] * vv[0] + cr[0]) + (p[1] * vv[1] + cr[1])
    proj = (inner / NPTS) / (square / NPTS + EPS)
    terms = []
    for i in range(2):
        off = p[i] - proj
        terms.append(e[i] + off * (2.0 * cr[i] + off * vv[i]))
    spread = jnp.sqrt(jnp.maximum(terms[0] + terms[1], 0.0) / NPTS + EPS)
    arnoldi_ref[0:1, :] = proj[:, 0:NRHS]
    arnoldi_ref[1:2, :] = spread[:, 0:NRHS]
    valid = lax.broadcasted_iota(jnp.int32, (1, 128), 1) < 16

    def tiled(x):
        x = jnp.where(valid, x, 0.0)
        for shift in (16, 32, 64):
            x = x + pltpu.roll(x, shift, 1)
        return x

    proj, spread = tiled(proj), tiled(spread)
    scalars_ref[0:1, :] = proj
    scalars_ref[1:2, :] = spread
    sums = mine_ref[0:4, :] + theirs_ref[0:4, :]
    chunk = (sums[0:2] - proj * sums[2:4]) / spread * math.sqrt(SKETCH / NPTS)
    for i in range(2):
        out_ref[pl.ds(4 + i, 128, stride=BACK_ROWS), :] = jnp.broadcast_to(
            chunk[i : i + 1], (128, 128)
        )


def last_kernel(got_ref, scalars_ref, v_ref, basis_hbm, sketch_hbm, turned, basis_ref, sketch_ref, sems):
    for half in range(2):
        tile = got_ref[pl.ds(4 + half, 128, stride=BACK_ROWS), :].T
        for t in range(8):
            sketch_ref[:, pl.ds((half * 8 + t) * 128, 128)] = tile[t * 16 : t * 16 + 16, :]
    copies = [pltpu.make_async_copy(sketch_ref, sketch_hbm, sems.at[8])]
    copies[0].start()
    proj = jnp.broadcast_to(scalars_ref[0:1, :], (128, 128)).T[0:NRHS, :]
    gain = jnp.broadcast_to(1.0 / scalars_ref[1:2, :], (128, 128)).T[0:NRHS, :]
    lane = lax.broadcasted_iota(jnp.int32, (32, 128), 1) & -16
    for c in range(4):
        blocks = []
        for jt in range(4):
            rows = got_ref[pl.ds(jt * 32 * BACK_ROWS + c, 32, stride=BACK_ROWS), :]
            blocks.append(pltpu.roll(rows, jt * 32, 1) if jt else rows)
        for m in range(8):
            made = blocks[0]
            for jt in range(1, 4):
                made = jnp.where(lane == (jt * 32 + m * 16) % 128, blocks[jt], made)
            made = pltpu.roll(made, 128 - m * 16, 1) if m else made
            turned[pl.ds(c * 8 + m, 32, stride=32), :] = made
    for jb in range(8):
        back = turned[pl.ds(jb * 128, 128), :].T
        for jt in range(4):
            cols = pl.ds((jb * 4 + jt) * 128, 128)
            x = back[jt * 32 : jt * 32 + 16, :]
            basis_ref[:, cols] = (x - proj * v_ref[:, cols]) * gain
        cols = pl.ds(jb * 512, 512)
        copies.append(
            pltpu.make_async_copy(basis_ref.at[:, cols], basis_hbm.at[:, cols], sems.at[jb])
        )
        copies[-1].start()
    for copy in copies:
        copy.wait()


VMEM = pl.BlockSpec(memory_space=pltpu.VMEM)
HBM = pl.BlockSpec(memory_space=pltpu.HBM)


def f32(*shape):
    return jax.ShapeDtypeStruct(shape, F32)


def call(kernel, out, ins, scratch=(), flops=1000000, mib=12, outs=None):
    single = not isinstance(out, tuple)
    return pl.pallas_call(
        kernel,
        out_shape=out,
        in_specs=ins,
        out_specs=outs or (VMEM if single else tuple(VMEM for _ in out)),
        scratch_shapes=list(scratch),
        cost_estimate=pl.CostEstimate(flops=flops, bytes_accessed=1000000, transcendentals=0),
        compiler_params=pltpu.CompilerParams(vmem_limit_bytes=mib * 1024 * 1024),
    )


def exchange(x):
    return lax.all_to_all(x[:, None, :], CHIP, 0, 0, tiled=True)[:, 0, :]


def body(basis_vector, diagonal, coords, phase_scale, sketch_rows, sketch_signs):
    chip = lax.axis_index(CHIP)
    core = lax.axis_index(CORE)
    info = jnp.stack([phase_scale[0] % MOD, chip, core] + [core] * 5).astype(jnp.int32)
    info = jnp.broadcast_to(info[:, None], (8, 128))
    points = LEAF * CHIPS
    swap = [(0, 1), (1, 0)]
    sketch_rows, sketch_signs = sketch_rows.reshape(32, 128), sketch_signs.reshape(32, 128)
    vector = pltpu.VMEM((NRHS, points), F32)
    ints = pltpu.VMEM((32, 128), jnp.int32)
    turned = pltpu.VMEM((1024, 128), F32)
    parts = pltpu.VMEM((256, points), jnp.bfloat16)
    hot_type = jax.ShapeDtypeStruct((256, points), jnp.bfloat16)
    packed = call(
        pack_kernel,
        f32(CHIPS * OUT_ROWS, 128),
        [HBM] * 5,
        [
            vector,
            pltpu.VMEM((2, points), jnp.int32),
            pltpu.VMEM((32, 128), F32),
            ints,
            ints,
            turned,
            pltpu.SemaphoreType.DMA((5,)),
        ],
        mib=60,
    )(basis_vector, coords, diagonal.reshape(32, 128), sketch_rows, sketch_signs)
    tile = f32(CHIPS, 128)
    maps, keep, give = call(
        early_kernel,
        (f32(SECTIONS - 1, 2, WIDTH, WIDTH, 128), tile, tile),
        [VMEM] + [HBM] * 3,
        [
            vector,
            ints,
            ints,
            pltpu.VMEM((SECTIONS - 1, 2, WIDTH, WIDTH, 128), F32),
            parts,
            parts,
            pltpu.SemaphoreType.DMA((3,)),
            pltpu.SemaphoreType.DMA((SECTIONS - 1,)),
        ],
        outs=(HBM, VMEM, VMEM),
        flops=20000000,
        mib=EARLY_MIB,
    )(info, basis_vector, sketch_rows, sketch_signs)
    got = exchange(packed)
    taken = lax.ppermute(give, CORE, swap)
    coeffs, leaf, held = call(
        leaf_kernel,
        (f32(512, 128), f32(WIDTH, LEAF, 128), f32(OUT_ROWS * 128, 128)),
        [VMEM, VMEM, HBM],
    )(info, got, keep)
    partner = lax.ppermute(coeffs, CORE, swap)
    first_type = f32(2, WIDTH, WIDTH, 128)
    hot, first = call(hot_kernel, (hot_type, first_type), [VMEM, VMEM])(info, held)
    pair = pltpu.VMEM((2, 512, 128), F32)
    parts_out, image = call(
        core_kernel,
        (f32(CHIPS * SUM_ROWS, 128), f32(512, 128)),
        [VMEM] * 8 + [HBM],
        [
            pair,
            pair,
            pltpu.VMEM((512, 128), F32),
            parts,
            pltpu.VMEM((3, 2, WIDTH, WIDTH, 128), F32),
            pltpu.SemaphoreType.DMA((3,)),
        ],
        mib=CORE_MIB,
    )(coeffs, partner, leaf, held, first, hot, keep, taken, maps)
    mine = call(sum_kernel, f32(8, 128), [VMEM, VMEM])(info, exchange(parts_out))
    theirs = lax.ppermute(mine, CORE, swap)
    back, arnoldi, scalars = call(
        chunk_kernel, (f32(CHIPS * BACK_ROWS, 128), f32(2, NRHS), f32(2, 128)), [VMEM] * 3
    )(mine, theirs, image)
    new_basis, sketch = call(
        last_kernel,
        (f32(NRHS, points), f32(NRHS, SKETCH)),
        [VMEM] * 3,
        [turned, vector, pltpu.VMEM((NRHS, SKETCH), F32), pltpu.SemaphoreType.DMA((9,))],
        outs=(HBM, HBM),
    )(exchange(back), scalars, basis_vector)
    return new_basis, sketch, arnoldi


def solution(mesh):
    torus = Mesh(mesh.devices.reshape(4, 8, 4, 2), ("box_0", "box_1", "box_2", "box_3"))
    box = ("box_0", "box_1", "box_2", "box_3")
    placed = (P(None, box), P(box), P(None, box), P(), P(box), P(box))
    return jax.shard_map(
        body, mesh=torus, in_specs=placed, out_specs=(P(None, box), P(), P()), check_vma=False
    )
```

```python
import functools
import math

import jax
import jax.numpy as jnp
from jax import lax
from jax.experimental import pallas as pl
from jax.experimental.pallas import tpu as pltpu
from jax.sharding import Mesh
from jax.sharding import PartitionSpec as P

RANK = 16
WIDTH = 32
LEAF = 32
SKETCH = 2048
NRHS = 16
SECTIONS = 8
CHIPS = 128
NPTS = 1048576
MOD = 8191
EPS = 1e-06
CHIP = ("box_0", "box_1", "box_2")
CORE = "box_3"
OUT_ROWS = 6
SUM_ROWS = 4
BACK_ROWS = 6
EARLY_MIB = 48
CORE_MIB = 47
F32 = jnp.float32


def fold(x):
    return (x & MOD) + (x >> 13)


def unit_circle(phase):
    r = phase.astype(F32)
    r = jnp.where(r > 4095.5, r - float(MOD), r)
    y = r * (math.pi / MOD)
    y2 = y * y
    s = 1.0 / math.factorial(13)
    for k in (11, 9, 7, 5, 3, 1):
        s = s * y2 + (-1.0) ** (k // 2) / math.factorial(k)
    s = s * y
    c = -1.0 / math.factorial(14)
    for k in (12, 10, 8, 6, 4, 2, 0):
        c = c * y2 + (-1.0) ** (k // 2) / math.factorial(k)
    return 1.0 - 2.0 * s * s, 2.0 * s * c


def times(a, b):
    return a[0] * b[0] - a[1] * b[1], a[0] * b[1] + a[1] * b[0]


def split_rows(lhs, y, high, cols):
    top = y.astype(jnp.bfloat16).astype(F32)
    for p, part in enumerate((top, y - top)):
        for h in range(8):
            mask = jnp.broadcast_to(high == h, (NRHS, 128))
            lhs[pl.ds(p * 128 + h * 16, 16), cols] = jnp.where(mask, part, 0.0).astype(jnp.bfloat16)


def hot_rows(rhs, low, cols):
    index = lax.broadcasted_iota(jnp.int32, (256, 128), 0)
    rhs[:, cols] = jnp.where(index == low, 1.0, 0.0).astype(jnp.bfloat16)


def sketched(lhs, rhs):
    both = lax.dot_general(
        lhs[...], rhs[...], (((1,), (1,)), ((), ())), preferred_element_type=F32
    )
    both = both[0:128] + both[128:256]
    return [
        jnp.concatenate(
            [
                both[(t // 2) * 16 : (t // 2) * 16 + 16, (t % 2) * 128 : (t % 2) * 128 + 128]
                for t in range(half * 8, half * 8 + 8)
            ],
            0,
        ).T
        for half in range(2)
    ]


def fetches(sources, held, sems):
    return [pltpu.make_async_copy(a, b, sems.at[i]) for i, (a, b) in enumerate(zip(sources, held))]


def pack_kernel(*refs):
    sources, out_ref, held, turned, sems = refs[:5], refs[5], refs[6:11], refs[11], refs[12]
    copies = fetches(sources, held, sems)
    for copy in copies:
        copy.start()
    for copy in copies:
        copy.wait()
    v_ref, coords_ref, diag_ref, rows_ref, signs_ref = held
    zeros = jnp.zeros((11, 128), F32)
    for jb in range(8):
        tiles = []
        for jt in range(4):
            j = jb * 4 + jt
            cols = pl.ds(j * 128, 128)
            tiles += [
                v_ref[:, cols],
                coords_ref[:, cols].astype(F32),
                diag_ref[j : j + 1, :],
                rows_ref[j : j + 1, :].astype(F32),
                signs_ref[j : j + 1, :].astype(F32),
                zeros,
            ]
        turned[pl.ds(jb * 128, 128), :] = jnp.concatenate(tiles, 0).T
    lane = lax.broadcasted_iota(jnp.int32, (32, 128), 1)
    made = {}
    for s in range(LEAF):
        rows = turned[pl.ds(s, 32, stride=32), :]
        for col, start, width, at in (
            (s // 8, 0, 16, 16 * (s % 8)),
            (4 + s // 16, 16, 8, 8 * (s % 16)),
        ):
            moved = pltpu.roll(rows, at, 1) if at else rows
            for jt in range(4):
                first = (jt * 32 + start + at) % 128
                if (col, jt) in made:
                    moved_here = jnp.where((lane & -width) == first, moved, made[col, jt])
                else:
                    moved_here = moved
                made[col, jt] = moved_here
    for (col, jt), rows in made.items():
        shift = (-jt * 32 - (16 if col >= 4 else 0)) % 128
        rows = pltpu.roll(rows, shift, 1) if shift else rows
        out_ref[pl.ds(jt * 32 * OUT_ROWS + col, 32, stride=OUT_ROWS), :] = rows


def product(out_count, terms, store, start=None, width=16, group=16):
    def tile(t, carry):
        accs = [jnp.zeros((8, 128), F32)] * (2 * width)
        if start is not None:
            accs = [x for i in range(width) for x in start(t * width + i)]

        def some(g, accs):
            accs = list(accs)
            for matrix, vector in terms:
                for i in range(group):
                    b = g * group + i
                    vec = vector(b)
                    for i in range(width):
                        row = jnp.broadcast_to(matrix(t * width + i, b), (8, 128))
                        for half in range(2):
                            accs[2 * i + half] += row * vec[half]
            return tuple(accs)

        accs = lax.fori_loop(0, 32 // group, some, tuple(accs))
        for i in range(width):
            store(t * width + i, accs[2 * i : 2 * i + 2])
        return carry

    lax.fori_loop(0, out_count // width, tile, 0)


def halves(ref, a, *lead):
    return [ref[(*lead, pl.ds(pl.multiple_of(a * 16 + 8 * h, 8), 8), slice(None))] for h in range(2)]


def row16(a):
    return pl.ds(pl.multiple_of(a * 16, 16), 16)


def leaf_kernel(info_ref, got_ref, after_ref, coeffs_ref, leaf_ref, points_ref):
    for c in range(6):
        points_ref[pl.ds(c * 128, 128), :] = got_ref[pl.ds(c, 128, stride=OUT_ROWS), :].T
    scale = info_ref[0:1, :]

    def powers(field):
        where = points_ref[pl.ds(512 + field, 32, stride=8), :].astype(jnp.int32)
        one = unit_circle(fold(fold(where * scale)))
        two = times(one, one)
        return [one, two, times(two, one), times(two, two)]

    first, second = powers(0), powers(1)
    gain = 1.0 / math.sqrt(LEAF)
    second = [(c * gain, s * gain) for c, s in second]
    for w in range(RANK):
        c, s = times(first[w % 4], second[w // 4])
        leaf_ref[w] = c
        leaf_ref[w + RANK] = s

    def store(a, x):
        coeffs_ref[row16(a), :] = jnp.concatenate(x, 0)

    product(
        WIDTH,
        [(lambda a, b: leaf_ref[a, pl.ds(b, 1), :], lambda b: halves(points_ref, b))],
        store,
    )


def section_map(map_ref, unit, offset, first_power, turn, gain):
    index = lax.broadcasted_iota(jnp.int32, (WIDTH, 128), 0) + offset
    one = unit_circle(fold(fold(unit * index)))
    two = times(one, one)
    four = times(two, two)
    scale = (gain * math.cos(turn), gain * math.sin(turn))
    power = one if first_power == 1 else times(two, one)
    power = (
        power[0] * scale[0] - power[1] * scale[1],
        power[0] * scale[1] + power[1] * scale[0],
    )
    fine = [power]
    for _ in range(3):
        fine.append(times(fine[-1], one))
    coarse = None
    for i in range(8):
        for j in range(4):
            c, s = fine[j]
            map_ref[4 * i + j] = c if coarse is None else coarse[0] * c - coarse[1] * s
        coarse = four if coarse is None else times(coarse, four)


def state_rows(parts):
    pad = [jnp.zeros((128 - 16 * len(parts), 128), F32)]
    return jnp.sum(jnp.concatenate(parts + pad, 0).T, axis=0, keepdims=True)


def section_maps(info_ref, k, maps_ref):
    scale, chip, core = info_ref[0:1, :], info_ref[1:2, :], info_ref[2:3, :]
    place = ((chip >> 2) & 7) * 16 + (chip >> 5) * 4 + (chip & 3)
    lane = lax.broadcasted_iota(jnp.int32, (1, 128), 1)
    key = ((lane * 2 + core) * 128 + place) * 37 + 101 * k
    whole = (key.astype(F32) * (1.0 / (MOD - 1))).astype(jnp.int32)
    key = key - whole * (MOD - 1)
    key = jnp.where(key < 0, key + (MOD - 1), key)
    key = jnp.where(key >= MOD - 1, key - (MOD - 1), key)
    unit = fold(fold((key + 1) * scale))
    turn = 2.0 * math.pi * 4096 / MOD
    section_map(maps_ref.at[0], unit, 2, 1, 0.0, 0.35 / math.sqrt(WIDTH))
    section_map(maps_ref.at[1], unit, 1, 3, turn, 0.6 / math.sqrt(WIDTH))


def early_kernel(info_ref, *refs):
    sources, maps_hbm, keep_ref, give_ref = refs[:3], *refs[3:6]
    held, maps, lhs, rhs, sems, map_sems = refs[6:9], *refs[9:]
    copies = fetches(sources, held, sems)
    for copy in copies:
        copy.start()

    def leave(k):
        return pltpu.make_async_copy(maps.at[k - 1], maps_hbm.at[k - 1], map_sems.at[k - 1])

    def section(k, carry):
        section_maps(info_ref, k, maps.at[k - 1])
        leave(k).start()
        return carry

    lax.fori_loop(1, SECTIONS, section, 0)
    for copy in copies:
        copy.wait()
    v_ref, rows_ref, signs_ref = held
    for j in range(32):
        cols = pl.ds(j * 128, 128)
        rows, signs = rows_ref[j : j + 1, :], signs_ref[j : j + 1, :]
        split_rows(lhs, v_ref[:, cols] * (2 * signs - 1).astype(F32), rows >> 8, cols)
        hot_rows(rhs, rows & 255, cols)
    low, high = sketched(lhs, rhs)
    first = info_ref[2:3, :] == 0
    first = jnp.broadcast_to(first, (128, 128))
    keep_ref[...] = jnp.where(first, low, high)
    give_ref[...] = jnp.where(first, high, low)
    for k in range(1, SECTIONS):
        leave(k).wait()


def hot_kernel(info_ref, points_ref, coeffs_ref, rhs_ref, maps_ref, begun_ref):
    for s in range(LEAF):
        low = points_ref[pl.ds(512 + s * 8 + 3, 1), :].astype(jnp.int32) & 255
        hot_rows(rhs_ref, low, pl.ds(s * 128, 128))
    section_maps(info_ref, 0, maps_ref)

    def store(a, x):
        begun_ref[row16(a), :] = jnp.concatenate(x, 0)

    product(
        WIDTH,
        [(lambda a, b: maps_ref[0, a, pl.ds(b, 1), :], lambda b: halves(coeffs_ref, b))],
        store,
        lambda a: [0.85 * x for x in halves(coeffs_ref, a)],
    )


def core_kernel(
    begun_ref,
    partner_ref,
    leaf_ref,
    points_ref,
    first,
    rhs,
    keep_ref,
    taken_ref,
    maps_hbm,
    out_ref,
    image_ref,
    now,
    other,
    image,
    lhs,
    maps,
    sems,
):
    lane = lax.broadcasted_iota(jnp.int32, (1, 128), 1)
    lanes = lax.broadcasted_iota(jnp.int32, (8, 128), 1)

    def copy(k):
        slot = lax.rem(k, 3)
        return pltpu.make_async_copy(maps_hbm.at[k - 1], maps.at[slot], sems.at[slot])

    copy(jnp.int32(1)).start()
    copy(jnp.int32(2)).start()

    def section(k, terms, start):
        at = k & 1
        step = jnp.left_shift(1, jnp.minimum(k, SECTIONS - 2))
        across = lanes ^ step

        def store(a, x):
            now[1 - at, row16(a), :] = jnp.concatenate(x, 0)
            other[1 - at, row16(a), :] = jnp.concatenate(
                [jnp.take_along_axis(y, across, axis=1, mode="promise_in_bounds") for y in x], 0
            )

        product(WIDTH, terms(at), store, start)

    section(
        jnp.int32(0),
        lambda at: [
            (lambda a, b: first[1, a, pl.ds(b, 1), :], lambda b: halves(partner_ref, b)),
        ],
        lambda a: halves(begun_ref, a),
    )

    def later(k, carry):
        copy(k).wait()

        @pl.when(k < SECTIONS - 2)
        def _():
            copy(k + 2).start()

        slot = lax.rem(k, 3)
        own, cross = maps.at[slot, 0], maps.at[slot, 1]
        section(
            k,
            lambda at: [
                (lambda a, b: own[a, pl.ds(b, 1), :], lambda b: halves(now, b, at)),
                (lambda a, b: cross[a, pl.ds(b, 1), :], lambda b: halves(other, b, at)),
            ],
            lambda a: [0.85 * x for x in halves(now, a, k & 1)],
        )
        return carry

    lax.fori_loop(1, SECTIONS, later, 0)

    def apply(s, x):
        at = pl.multiple_of(512 + s * 8, 8)
        diagonal = points_ref[pl.ds(at, 8), :][2:3, :]
        image[row16(s), :] = diagonal * points_ref[row16(s), :] + jnp.concatenate(x, 0)

    product(
        LEAF,
        [(lambda a, b: leaf_ref[b, pl.ds(a, 1), :], lambda b: halves(now, b, 0))],
        apply,
    )
    square = jnp.zeros((NRHS, 128), F32)
    inner = jnp.zeros((NRHS, 128), F32)
    for s in range(LEAF):
        v = points_ref[pl.ds(s * 16, 16), :]
        x = image[pl.ds(s * 16, 16), :]
        square += v * v
        inner += v * x
        sign = 2.0 * points_ref[pl.ds(512 + s * 8 + 4, 1), :] - 1.0
        high = points_ref[pl.ds(512 + s * 8 + 3, 1), :].astype(jnp.int32) >> 8
        split_rows(lhs, x * sign, high, pl.ds(s * 128, 128))
    sums = state_rows([square, inner])
    valid = lane < 16
    vv = jnp.where(valid, sums, 0.0)
    iv = jnp.where(valid, pltpu.roll(sums, 112, 1), 0.0)
    local = jnp.where(vv > 0.0, iv / jnp.where(vv > 0.0, vv, 1.0), 0.0)
    across = jnp.broadcast_to(local, (128, 128)).T[0:NRHS, :]
    energy = jnp.zeros((NRHS, 128), F32)
    mixed = jnp.zeros((NRHS, 128), F32)
    for s in range(LEAF):
        v = points_ref[pl.ds(s * 16, 16), :]
        r = image[pl.ds(s * 16, 16), :] - across * v
        energy += r * r
        mixed += r * v
    for c in range(4):
        image_ref[pl.ds(c, 128, stride=BACK_ROWS), :] = image[pl.ds(c * 128, 128), :].T
    for half, tile in enumerate(sketched(lhs, rhs)):
        out_ref[pl.ds(half, 128, stride=SUM_ROWS), :] = tile
    out_ref[pl.ds(2, 128, stride=SUM_ROWS), :] = keep_ref[...] + taken_ref[...]
    rest = jnp.where(lane < 32, state_rows([energy, mixed]), 0.0)
    state = vv + pltpu.roll(local, 16, 1) + pltpu.roll(rest, 32, 1)
    out_ref[pl.ds(3, 128, stride=SUM_ROWS), :] = jnp.broadcast_to(state, (128, 128))


def merged(vv, p, e, cr, total):
    square = total(vv)
    inner = total(p * vv + cr)
    local = jnp.where(square > 0.0, inner / jnp.where(square > 0.0, square, 1.0), 0.0)
    return square, inner, local


def moved_energy(vv, p, e, cr, at, total):
    off = p - at
    return total(e + off * (2.0 * cr + off * vv)), total(cr + off * vv)


def sum_kernel(info_ref, got_ref, out_ref):
    sums = [
        jnp.sum(got_ref[pl.ds(c, 128, stride=SUM_ROWS), :], axis=0, keepdims=True)
        for c in range(3)
    ]
    first = info_ref[2:3, :] == 0
    out_ref[0:1, :] = sums[0]
    out_ref[1:2, :] = sums[1]
    out_ref[2:3, :] = jnp.where(first, sums[2], 0.0)
    out_ref[3:4, :] = jnp.where(first, 0.0, sums[2])
    state = got_ref[pl.ds(3, 128, stride=SUM_ROWS), :]
    valid = lax.broadcasted_iota(jnp.int32, (128, 128), 1) < 16
    parts = [
        jnp.where(valid, pltpu.roll(state, (128 - 16 * i) % 128, 1) if i else state, 0.0)
        for i in range(4)
    ]

    def total(x):
        return jnp.sum(x, axis=0, keepdims=True)

    square, inner, local = merged(*parts, total)
    energy, mixed = moved_energy(*parts, local, total)
    for i, x in enumerate((square, local, energy, mixed)):
        out_ref[4 + i : 5 + i, :] = x


def chunk_kernel(mine_ref, theirs_ref, image_ref, out_ref, arnoldi_ref, scalars_ref):
    both = [(mine_ref[4 + i : 5 + i, :], theirs_ref[4 + i : 5 + i, :]) for i in range(4)]
    vv, p, e, cr = both
    square = vv[0] + vv[1]
    inner = (p[0] * vv[0] + cr[0]) + (p[1] * vv[1] + cr[1])
    proj = (inner / NPTS) / (square / NPTS + EPS)
    terms = []
    for i in range(2):
        off = p[i] - proj
        terms.append(e[i] + off * (2.0 * cr[i] + off * vv[i]))
    spread = jnp.sqrt(jnp.maximum(terms[0] + terms[1], 0.0) / NPTS + EPS)
    arnoldi_ref[0:1, :] = proj[:, 0:NRHS]
    arnoldi_ref[1:2, :] = spread[:, 0:NRHS]
    valid = lax.broadcasted_iota(jnp.int32, (1, 128), 1) < 16

    def tiled(x):
        x = jnp.where(valid, x, 0.0)
        for shift in (16, 32, 64):
            x = x + pltpu.roll(x, shift, 1)
        return x

    proj, spread = tiled(proj), tiled(spread)
    scalars_ref[0:1, :] = proj
    scalars_ref[1:2, :] = spread
    sums = mine_ref[0:4, :] + theirs_ref[0:4, :]
    chunk = (sums[0:2] - proj * sums[2:4]) / spread * math.sqrt(SKETCH / NPTS)
    for i in range(2):
        out_ref[pl.ds(4 + i, 128, stride=BACK_ROWS), :] = jnp.broadcast_to(
            chunk[i : i + 1], (128, 128)
        )


def last_kernel(got_ref, scalars_ref, v_ref, basis_hbm, sketch_hbm, turned, basis_ref, sketch_ref, sems):
    for half in range(2):
        tile = got_ref[pl.ds(4 + half, 128, stride=BACK_ROWS), :].T
        for t in range(8):
            sketch_ref[:, pl.ds((half * 8 + t) * 128, 128)] = tile[t * 16 : t * 16 + 16, :]
    copies = [pltpu.make_async_copy(sketch_ref, sketch_hbm, sems.at[8])]
    copies[0].start()
    proj = jnp.broadcast_to(scalars_ref[0:1, :], (128, 128)).T[0:NRHS, :]
    gain = jnp.broadcast_to(1.0 / scalars_ref[1:2, :], (128, 128)).T[0:NRHS, :]
    lane = lax.broadcasted_iota(jnp.int32, (32, 128), 1) & -16
    for c in range(4):
        blocks = []
        for jt in range(4):
            rows = got_ref[pl.ds(jt * 32 * BACK_ROWS + c, 32, stride=BACK_ROWS), :]
            blocks.append(pltpu.roll(rows, jt * 32, 1) if jt else rows)
        for m in range(8):
            made = blocks[0]
            for jt in range(1, 4):
                made = jnp.where(lane == (jt * 32 + m * 16) % 128, blocks[jt], made)
            made = pltpu.roll(made, 128 - m * 16, 1) if m else made
            turned[pl.ds(c * 8 + m, 32, stride=32), :] = made
    for jb in range(8):
        back = turned[pl.ds(jb * 128, 128), :].T
        for jt in range(4):
            cols = pl.ds((jb * 4 + jt) * 128, 128)
            x = back[jt * 32 : jt * 32 + 16, :]
            basis_ref[:, cols] = (x - proj * v_ref[:, cols]) * gain
        cols = pl.ds(jb * 512, 512)
        copies.append(
            pltpu.make_async_copy(basis_ref.at[:, cols], basis_hbm.at[:, cols], sems.at[jb])
        )
        copies[-1].start()
    for copy in copies:
        copy.wait()


VMEM = pl.BlockSpec(memory_space=pltpu.VMEM)
HBM = pl.BlockSpec(memory_space=pltpu.HBM)


def f32(*shape):
    return jax.ShapeDtypeStruct(shape, F32)


def call(kernel, out, ins, scratch=(), flops=1000000, mib=12, outs=None, alias=None):
    single = not isinstance(out, tuple)
    return pl.pallas_call(
        kernel,
        out_shape=out,
        in_specs=ins,
        out_specs=outs or (VMEM if single else tuple(VMEM for _ in out)),
        scratch_shapes=list(scratch),
        input_output_aliases=alias or {},
        cost_estimate=pl.CostEstimate(flops=flops, bytes_accessed=1000000, transcendentals=0),
        compiler_params=pltpu.CompilerParams(vmem_limit_bytes=mib * 1024 * 1024),
    )


def exchange(x):
    return lax.all_to_all(x[:, None, :], CHIP, 0, 0, tiled=True)[:, 0, :]


def body(basis_vector, diagonal, coords, phase_scale, sketch_rows, sketch_signs):
    chip = lax.axis_index(CHIP)
    core = lax.axis_index(CORE)
    info = jnp.stack([phase_scale[0] % MOD, chip, core] + [core] * 5).astype(jnp.int32)
    info = jnp.broadcast_to(info[:, None], (8, 128))
    points = LEAF * CHIPS
    swap = [(0, 1), (1, 0)]
    sketch_rows, sketch_signs = sketch_rows.reshape(32, 128), sketch_signs.reshape(32, 128)
    vector = pltpu.VMEM((NRHS, points), F32)
    ints = pltpu.VMEM((32, 128), jnp.int32)
    turned = pltpu.VMEM((1024, 128), F32)
    parts = pltpu.VMEM((256, points), jnp.bfloat16)
    hot_type = jax.ShapeDtypeStruct((256, points), jnp.bfloat16)
    packed = call(
        pack_kernel,
        f32(CHIPS * OUT_ROWS, 128),
        [HBM] * 5,
        [
            vector,
            pltpu.VMEM((2, points), jnp.int32),
            pltpu.VMEM((32, 128), F32),
            ints,
            ints,
            turned,
            pltpu.SemaphoreType.DMA((5,)),
        ],
        mib=60,
    )(basis_vector, coords, diagonal.reshape(32, 128), sketch_rows, sketch_signs)
    tile = f32(CHIPS, 128)
    maps, keep, give = call(
        early_kernel,
        (f32(SECTIONS - 1, 2, WIDTH, WIDTH, 128), tile, tile),
        [VMEM] + [HBM] * 3,
        [
            vector,
            ints,
            ints,
            pltpu.VMEM((SECTIONS - 1, 2, WIDTH, WIDTH, 128), F32),
            parts,
            parts,
            pltpu.SemaphoreType.DMA((3,)),
            pltpu.SemaphoreType.DMA((SECTIONS - 1,)),
        ],
        outs=(HBM, VMEM, VMEM),
        flops=20000000,
        mib=EARLY_MIB,
    )(info, basis_vector, sketch_rows, sketch_signs)
    got = exchange(packed)
    taken = lax.ppermute(give, CORE, swap)
    coeffs, leaf, held = call(
        leaf_kernel,
        (f32(512, 128), f32(WIDTH, LEAF, 128), f32(OUT_ROWS * 128, 128)),
        [VMEM, VMEM, HBM],
    )(info, got, taken)
    partner = lax.ppermute(coeffs, CORE, swap)
    first_type = f32(2, WIDTH, WIDTH, 128)
    hot, first, begun = call(
        hot_kernel, (hot_type, first_type, f32(512, 128)), [VMEM] * 3
    )(info, held, coeffs)
    pair = pltpu.VMEM((2, 512, 128), F32)
    parts_out, image = call(
        core_kernel,
        (f32(CHIPS * SUM_ROWS, 128), f32(CHIPS * BACK_ROWS, 128)),
        [VMEM] * 8 + [HBM],
        [
            pair,
            pair,
            pltpu.VMEM((512, 128), F32),
            parts,
            pltpu.VMEM((3, 2, WIDTH, WIDTH, 128), F32),
            pltpu.SemaphoreType.DMA((3,)),
        ],
        mib=CORE_MIB,
    )(begun, partner, leaf, held, first, hot, keep, taken, maps)
    mine = call(sum_kernel, f32(8, 128), [VMEM, VMEM])(info, exchange(parts_out))
    theirs = lax.ppermute(mine, CORE, swap)
    back, arnoldi, scalars = call(
        chunk_kernel,
        (f32(CHIPS * BACK_ROWS, 128), f32(2, NRHS), f32(2, 128)),
        [VMEM] * 3,
        alias={2: 0},
    )(mine, theirs, image)
    new_basis, sketch = call(
        last_kernel,
        (f32(NRHS, points), f32(NRHS, SKETCH)),
        [VMEM] * 3,
        [turned, vector, pltpu.VMEM((NRHS, SKETCH), F32), pltpu.SemaphoreType.DMA((9,))],
        outs=(HBM, HBM),
    )(exchange(back), scalars, basis_vector)
    return new_basis, sketch, arnoldi


def solution(mesh):
    torus = Mesh(mesh.devices.reshape(4, 8, 4, 2), ("box_0", "box_1", "box_2", "box_3"))
    box = ("box_0", "box_1", "box_2", "box_3")
    placed = (P(None, box), P(box), P(None, box), P(), P(box), P(box))
    return jax.shard_map(
        body, mesh=torus, in_specs=placed, out_specs=(P(None, box), P(), P()), check_vma=False
    )
```
